32 devices in a mesh: grp: 2 (over y), lay: 4 (over z), wid: 2 (over x), rep: 2 (over core).
Axes of the slice: x: 2, y: 2, z: 4, core: 2. Of those that a mesh axis runs over, the one named last changes fastest.
Arguments:
- acts: bfloat16 [4, 1024, 2048], P(None, ('grp', 'rep'), 'wid'), parts along dimension 1, may hold values from -6 to 6
- targets: bfloat16 [4, 1024, 2048], P(None, ('grp', 'rep'), 'wid'), parts along dimension 1, may hold values from -6 to 6
- enc_weight: bfloat16 [2048, 8192], P('wid', 'lay'), may hold values from -0.125 to 0.125
- enc_bias: float32 [8192], P('lay'), may hold values from -3 to 3
- gate_mask: int32 [1024, 32], P(('grp', 'rep'), 'lay'), parts along dimension 0, may hold values 0 or 1
- dec_list: int32 [84, 3], P('lay'), may hold values from -1 to 7, as said below
- dec_weight: bfloat16 [84, 256, 2048], P('lay', None, 'wid'), may hold values from -0.125 to 0.125
Outputs:
- grad_enc: float32 [4096, 8192], P(('grp', 'wid'), ('lay', 'rep')), parts along dimension 0
- grad_bias: float32 [16384], P(('grp', 'lay', 'rep')), parts along dimension 0
- grad_dec: float32 [168, 256, 2048], P(('grp', 'lay'), 'rep', 'wid'), parts along dimension 0
The draws below stay inside these ranges and needn't reach their ends.
There are 2 independent parts, one for each index of `grp`. The reference program is written for one: setup_inputs(seed, part) draws one part's arguments, and reference() takes and returns one part's arrays. A program takes and returns all parts, laid end to end along the dimension named above; an argument that names none is the same for every part. Nothing has to cross between parts.
Inputs may be any that keep to these rules, and one draw needn't show every extreme that they name: `dec_list`: each row is (source layer, target layer, latent block within the layer's slab); every triple with source <= target < 4 and block < 8 stands in exactly one row; every other row is (-1, -1, -1).
All inputs are finite; a program needn't handle non-finite values. No bound on the sum of `gate_mask` on one device may be relied on, other than what follows from the above.
Results may differ from the reference program's by a relative error of at most 0.019.
Values may be sent and summed in bfloat16 or wider, within the bound.
A program may use at most 128 MiB of HBM per device.

```python
import jax
import jax.numpy as jnp
import numpy as np
from jax import lax

D = 2048
F = 2048
L = 4
BLK = 256
TOKENS = 512
NLB = 32
SLOTS = 21
N_LAY = 4


def draw_dec_list(key, part):
    blocks_layer = F // BLK
    triples = np.array([[source_layer, target_layer, within] for source_layer in range(L) for target_layer in range(source_layer, L) for within in range(blocks_layer)], dtype=np.int32)
    placing = jax.random.permutation(jax.random.fold_in(key, 11), N_LAY * SLOTS)
    filled = jnp.full((N_LAY * SLOTS, 3), -1, jnp.int32)
    return filled.at[placing[:triples.shape[0]]].set(jnp.asarray(triples))


def with_ends(values, own_key, least, largest):
    index_at = [jax.random.randint(jax.random.fold_in(own_key, axis), (), 0, length) for axis, length in enumerate(values.shape)]
    widest = values.shape.index(max(values.shape))
    beside = index_at[:widest] + [(index_at[widest] + 1) % values.shape[widest]] + index_at[widest + 1:]
    return values.at[tuple(index_at)].set(least).at[tuple(beside)].set(largest)


def levels(rng, shape, shards, low, largest):
    def one(axis_at, parts):
        steps = jax.random.uniform(jax.random.fold_in(jax.random.fold_in(rng, 6), axis_at), (parts,), jnp.float32, low / len(shards), largest / len(shards))
        return jnp.repeat(jnp.exp(steps), shape[axis_at] // parts).reshape((-1,) + (1,) * (len(shape) - axis_at - 1))

    loudness = one(*shards[0])
    for cut in shards[1:]:
        loudness = loudness * one(*cut)
    return loudness


def bell_draw(key, shape, scale, limit, pieces=(), kind=jnp.bfloat16):
    level = levels(key, shape, pieces, -0.22, 0.18) if pieces else 1.0
    drawn = jax.random.normal(key, shape, jnp.float32) * scale * level
    return jnp.minimum(jnp.maximum(drawn, -limit), limit).astype(kind)


def setup_inputs(seed: int = 0, part: int = 0) -> dict:
    keys = jax.random.split(jax.random.key(seed), 8)
    part_keys = jax.random.split(jax.random.fold_in(keys[7], part), 8)
    return {
        "acts": bell_draw(part_keys[0], (L, TOKENS, D), 1.0, 6.0, ((1, 2), (2, 2))),
        "targets": bell_draw(part_keys[1], (L, TOKENS, D), 1.0, 6.0, ((1, 2), (2, 2))),
        "enc_weight": bell_draw(keys[2], (D, L * F), D ** -0.5, 0.125, ((0, 2), (1, 4))),
        "enc_bias": bell_draw(keys[3], (L * F,), 0.5, 3.0, ((0, 4),), jnp.float32),
        "gate_mask": with_ends((jax.random.randint(part_keys[4], (TOKENS, NLB), 0, 2) < 1).astype(jnp.int32), jax.random.fold_in(part_keys[4], 1), 0, 1),
        "dec_list": draw_dec_list(jax.random.fold_in(keys[7], 71), part),
        "dec_weight": bell_draw(keys[6], (N_LAY * SLOTS, BLK, D), F ** -0.5, 0.125, ((0, 4), (2, 2))),
    }


ROOT = 0.7978845608028654
CUBIC = 0.044715


def smooth_gate(shifted):
    inside_arg = ROOT * (shifted + CUBIC * shifted * shifted * shifted)
    return 0.5 * shifted * (1.0 + jnp.tanh(inside_arg))


def gate_slope(shifted):
    inside_arg = ROOT * (shifted + CUBIC * shifted * shifted * shifted)
    tanh_part = jnp.tanh(inside_arg)
    return 0.5 * (1.0 + tanh_part) + 0.5 * shifted * (1.0 - tanh_part * tanh_part) * ROOT * (1.0 + 3.0 * CUBIC * shifted * shifted)


def slot_tables(slot_entry, blocks_layer, blocks_total):
    block_id = slot_entry[:, 0] * blocks_layer + slot_entry[:, 2]
    target_layer = slot_entry[:, 1]
    slot_valid = (target_layer >= 0).astype(jnp.float32)
    target_hot = (target_layer[:, None] == jnp.arange(L, dtype=jnp.int32)[None, :]).astype(jnp.float32)
    block_hot = (block_id[:, None] == jnp.arange(blocks_total, dtype=jnp.int32)[None, :]).astype(jnp.float32)
    return block_id, target_layer, slot_valid, target_hot, block_hot


def reference(acts, targets, enc_weight, enc_bias, gate_mask, dec_list, dec_weight):
    blocks_layer = F // BLK
    blocks_total = L * blocks_layer
    tokens = acts.shape[1]
    pre_act = jnp.concatenate([jnp.dot(acts[layer_index], enc_weight[:, layer_index * F:(layer_index + 1) * F], preferred_element_type=jnp.float32) for layer_index in range(L)], axis=1)
    shifted = (pre_act + enc_bias.astype(jnp.float32)[None, :]).reshape(tokens, blocks_total, BLK)
    keep_mask = gate_mask.astype(jnp.float32)[:, :, None]
    latent = (smooth_gate(shifted) * keep_mask).astype(jnp.bfloat16)
    lists = dec_list.reshape(N_LAY, SLOTS, 3)
    weights = dec_weight.reshape(N_LAY, SLOTS, BLK, D)

    def forward_step(running, slot_pair):
        slot_entry, weight = slot_pair
        block_id, target_layer, slot_valid, target_hot, block_hot = slot_tables(slot_entry, blocks_layer, blocks_total)
        slot_lat = jnp.take(latent, jnp.maximum(block_id, 0), axis=1).astype(jnp.float32)
        contrib = jnp.einsum('tkb,kbd->ktd', slot_lat, weight.astype(jnp.float32), precision=lax.Precision.HIGHEST)
        return running + jnp.einsum('kl,ktd->ltd', target_hot, contrib, precision=lax.Precision.HIGHEST), None

    recon, _ = lax.scan(forward_step, jnp.zeros((L, tokens, D), jnp.float32), (lists, weights))
    scaled_error = ((recon - targets.astype(jnp.float32)) * (tokens ** -0.5)).astype(jnp.bfloat16)

    def backward_step(running, slot_pair):
        slot_entry, weight = slot_pair
        block_id, target_layer, slot_valid, target_hot, block_hot = slot_tables(slot_entry, blocks_layer, blocks_total)
        slot_lat = jnp.take(latent, jnp.maximum(block_id, 0), axis=1).astype(jnp.float32)
        err_slot = jnp.take(scaled_error, jnp.maximum(target_layer, 0), axis=0).astype(jnp.float32)
        dec_grad = jnp.einsum('tkb,ktd->kbd', slot_lat, err_slot, precision=lax.Precision.HIGHEST) * slot_valid[:, None, None]
        slot_error = jnp.einsum('ktd,kbd->tkb', err_slot, weight.astype(jnp.float32), precision=lax.Precision.HIGHEST)
        outgoing = jnp.einsum('tkb,kg->tgb', slot_error, block_hot, precision=lax.Precision.HIGHEST).astype(jnp.bfloat16)
        return running + outgoing.astype(jnp.float32), dec_grad

    latent_error, dec_grads = lax.scan(backward_step, jnp.zeros((tokens, blocks_total, BLK), jnp.float32), (lists, weights))
    pre_grad = (latent_error * keep_mask * gate_slope(shifted)).astype(jnp.bfloat16).reshape(tokens, L * F)
    grad_enc = jnp.concatenate([jnp.dot(acts[layer_index].T, pre_grad[:, layer_index * F:(layer_index + 1) * F], preferred_element_type=jnp.float32) for layer_index in range(L)], axis=1)
    grad_bias = jnp.sum(pre_grad.astype(jnp.float32), axis=0)
    grad_dec = dec_grads.reshape(N_LAY * SLOTS, BLK, D)
    return grad_enc, grad_bias, grad_dec
```

```python
import jax
import jax.numpy as jnp
from jax import lax
from jax.experimental import pallas as pl
from jax.experimental.pallas import tpu as pltpu
from jax.sharding import PartitionSpec as P

ROOT = 0.7978845608028654
CUBIC = 0.044715
MESH = pl.DeviceIdType.MESH
BF16 = jnp.bfloat16
F32 = jnp.float32
CUTS = 2
SKEW = 3


def smooth_gate(shifted):
    inside_arg = ROOT * (shifted + CUBIC * shifted * shifted * shifted)
    return 0.5 * shifted * (1.0 + jnp.tanh(inside_arg))


def gate_slope(shifted):
    inside_arg = ROOT * (shifted + CUBIC * shifted * shifted * shifted)
    tanh_part = jnp.tanh(inside_arg)
    return 0.5 * (1.0 + tanh_part) + 0.5 * shifted * (1.0 - tanh_part * tanh_part) * ROOT * (
        1.0 + 3.0 * CUBIC * shifted * shifted
    )


def loop(first, count, step):
    if count <= 4:
        for d in range(first, count):
            step(d)
    else:
        lax.fori_loop(first, count, lambda d, c: (step(d), c)[1], 0)


def others(me, count, step):
    loop(1, count, lambda d: step(lax.rem(me + d, count)))


def signal(barrier, **where):
    pl.semaphore_signal(barrier, inc=1, device_id=where, device_id_type=MESH)


def remote(src, dst, send_sem, recv_sem, **where):
    return pltpu.make_async_remote_copy(
        src_ref=src, dst_ref=dst, send_sem=send_sem, recv_sem=recv_sem, device_id=where,
        device_id_type=MESH,
    )


ANY = pl.BlockSpec(memory_space=pl.ANY)


def bounce(src, dst, held, sem):
    into = pltpu.make_async_copy(src, held, sem)
    into.start()
    into.wait()
    out = pltpu.make_async_copy(held, dst, sem)
    out.start()
    return out


def nearest(l, n, step):
    def both(d):
        for j in (l - d, l + d):

            @pl.when((j >= 0) & (j < n))
            def _():
                step(j)

    loop(1, n, both)


def line_gather(l, n, src, slot, send_sem, recv_sem, arrived):
    def own(step):
        @pl.when(l < n - 1)
        def _():
            step(remote(src, slot(l), send_sem.at[l], recv_sem.at[l], lay=l + 1))

        @pl.when(l > 0)
        def _():
            step(remote(src, slot(l), send_sem.at[n], recv_sem.at[l], lay=l - 1))

    def hop(j, step):
        @pl.when((j < l) & (l < n - 1))
        def _():
            step(remote(slot(j), slot(j), send_sem.at[j], recv_sem.at[j], lay=l + 1))

        @pl.when((j > l) & (l > 0))
        def _():
            step(remote(slot(j), slot(j), send_sem.at[j], recv_sem.at[j], lay=l - 1))

    def take(j):
        remote(slot(j), slot(j), send_sem.at[j], recv_sem.at[j], lay=j).wait_recv()
        hop(j, lambda c: c.start())
        arrived(j)

    def finish():
        own(lambda c: c.wait_send())
        nearest(l, n, lambda j: hop(j, lambda c: c.wait_send()))

    own(lambda c: c.start())
    return lambda: nearest(l, n, take), finish


def comm(body, args, outs, sems, cid, held=()):
    return pl.pallas_call(
        body,
        out_shape=tuple(outs),
        in_specs=[ANY] * len(args),
        out_specs=tuple([ANY] * len(outs)),
        scratch_shapes=[pltpu.SemaphoreType.DMA((s,)) for s in sems] + [pltpu.VMEM(*h) for h in held],
        compiler_params=pltpu.CompilerParams(collective_id=cid, has_side_effects=True),
        name=f"exchange_{cid}",
    )(*args)


def exchange(axis, x, out_shape, held_shape, src_of, dst_of, cid):
    n = lax.axis_size(axis)

    def body(x_ref, o_ref, ssem, rsem, lsem, held):
        me = lax.axis_index(axis)
        barrier = pltpu.get_barrier_semaphore()
        others(me, n, lambda j: signal(barrier, **{axis: j}))
        pl.semaphore_wait(barrier, n - 1)

        def send(j):
            return remote(
                src_of(x_ref, j), dst_of(o_ref, me), ssem.at[j], rsem.at[me], **{axis: j}
            )

        def arrival(j):
            return remote(
                src_of(x_ref, me), dst_of(o_ref, j), ssem.at[j], rsem.at[j], **{axis: j}
            )

        others(me, n, lambda j: send(j).start())
        own = bounce(src_of(x_ref, me), dst_of(o_ref, me), held, lsem.at[0])
        others(me, n, lambda j: arrival(j).wait_recv())
        others(me, n, lambda j: send(j).wait_send())
        own.wait()

    return comm(
        body, [x], [jax.ShapeDtypeStruct(out_shape, x.dtype)], (n, n, 1), cid,
        [(held_shape, x.dtype)],
    )[0]


def gather_latents(h, cid):
    n, w_count = lax.axis_size("lay"), lax.axis_size("wid")
    blocks, toks, width = h.shape

    def body(h_ref, o_ref, zs, zr, xs, xr, lsem, held):
        l, w = lax.axis_index("lay"), lax.axis_index("wid")
        barrier = pltpu.get_barrier_semaphore()
        others(l, n, lambda j: signal(barrier, lay=j))
        others(w, w_count, lambda v: signal(barrier, wid=v))
        pl.semaphore_wait(barrier, n + w_count - 2)

        def slot(j, v):
            return o_ref.at[pl.ds(j * blocks, blocks), v]

        def x_own(v):
            return remote(h_ref, slot(l, w), xs.at[l * w_count + v], xr.at[l * w_count + w], wid=v)

        def x_copy(j, v, source):
            return remote(
                slot(j, source), slot(j, source), xs.at[j * w_count + v],
                xr.at[j * w_count + source], wid=v,
            )

        take, finish = line_gather(
            l, n, h_ref, lambda j: slot(j, w), zs, zr,
            lambda j: others(w, w_count, lambda v: x_copy(j, v, w).start()),
        )
        others(w, w_count, lambda v: x_own(v).start())
        own = bounce(h_ref, slot(l, w), held, lsem.at[0])
        take()
        finish()
        others(w, w_count, lambda v: x_own(v).wait_send())
        nearest(l, n, lambda j: others(w, w_count, lambda v: x_copy(j, v, w).wait_send()))
        loop(0, n, lambda j: others(w, w_count, lambda v: x_copy(j, v, v).wait_recv()))
        own.wait()

    out = jax.ShapeDtypeStruct((n * blocks, w_count, toks, width), h.dtype)
    return comm(
        body, [h], [out], (n + 1, n, n * w_count, n * w_count, 1), cid, [(h.shape, h.dtype)]
    )[0]


def slots_and_twin(slot_err, lat, err, acts_here, cid):
    w_count, r_count = lax.axis_size("wid"), lax.axis_size("rep")
    assert r_count == 2
    slots, _, toks, width = slot_err.shape
    half = width // r_count

    def body(s_ref, l_ref, e_ref, a_ref, so_ref, lo_ref, eo_ref, ao_ref, ssem, rsem, lsem, ts, tr,
             held, held_acts):
        w, r = lax.axis_index("wid"), lax.axis_index("rep")
        twin = 1 - r
        barrier = pltpu.get_barrier_semaphore()
        others(w, w_count, lambda v: signal(barrier, wid=v))
        signal(barrier, rep=twin)
        pl.semaphore_wait(barrier, w_count)

        def send(v):
            return remote(s_ref.at[:, v], so_ref.at[w], ssem.at[v], rsem.at[w], wid=v)

        def arrival(v):
            return remote(s_ref.at[:, w], so_ref.at[v], ssem.at[v], rsem.at[v], wid=v)

        others(w, w_count, lambda v: send(v).start())
        twins = [
            remote(l_ref.at[:, :, pl.ds(pl.multiple_of(twin * half, half), half)], lo_ref,
                   ts.at[0], tr.at[0], rep=twin),
            remote(e_ref, eo_ref, ts.at[1], tr.at[1], rep=twin),
            remote(a_ref, ao_ref.at[r], ts.at[2], tr.at[2], rep=twin),
        ]
        for c in twins:
            c.start()
        own = bounce(s_ref.at[:, w], so_ref.at[w], held, lsem.at[0])
        own_acts = bounce(a_ref, ao_ref.at[r], held_acts, lsem.at[1])
        others(w, w_count, lambda v: arrival(v).wait_recv())
        others(w, w_count, lambda v: send(v).wait_send())
        own.wait()
        own_acts.wait()
        for c in twins:
            c.wait()

    outs = [
        jax.ShapeDtypeStruct((w_count, slots, toks, width), slot_err.dtype),
        jax.ShapeDtypeStruct(lat.shape[:2] + (half,), lat.dtype),
        jax.ShapeDtypeStruct(err.shape, err.dtype),
        jax.ShapeDtypeStruct((r_count,) + acts_here.shape, acts_here.dtype),
    ]
    return comm(body, [slot_err, lat, err, acts_here], outs, (w_count, w_count, 2, 3, 3), cid,
                [((slots, toks, width), slot_err.dtype), (acts_here.shape, acts_here.dtype)])


def gather_pre_grad(pg, cid):
    w_count, r_count = lax.axis_size("wid"), lax.axis_size("rep")
    _, toks, columns = pg.shape

    def body(p_ref, o_ref, ssem, rsem, lsem, held):
        w, r = lax.axis_index("wid"), lax.axis_index("rep")
        barrier = pltpu.get_barrier_semaphore()

        def peers(step):
            others(w, w_count, lambda v: loop(0, r_count, lambda q: step(v, q)))
            others(r, r_count, lambda q: step(w, q))

        peers(lambda v, q: signal(barrier, wid=v, rep=q))
        pl.semaphore_wait(barrier, w_count * r_count - 1)

        def send(v, q):
            return remote(p_ref.at[q], o_ref.at[r, w], ssem.at[q * w_count + v],
                          rsem.at[r * w_count + w], wid=v, rep=q)

        def arrival(v, q):
            return remote(p_ref.at[q], o_ref.at[q, v], ssem.at[q * w_count + v],
                          rsem.at[q * w_count + v], wid=v, rep=q)

        peers(lambda v, q: send(v, q).start())
        own = bounce(p_ref.at[r], o_ref.at[r, w], held, lsem.at[0])
        peers(lambda v, q: arrival(v, q).wait_recv())
        peers(lambda v, q: send(v, q).wait_send())
        own.wait()

    out = jax.ShapeDtypeStruct((r_count, w_count, toks, columns), pg.dtype)
    total = w_count * r_count
    return comm(
        body, [pg], [out], (total, total, 1), cid, [((toks, columns), pg.dtype)]
    )[0]


def group_of(slots):
    return 3 if slots % 3 == 0 else 1


def slot_call(body, tables, args, in_specs, out_shape, out_spec, scratch, flops, name, grid):
    moved = sum(a.size * a.dtype.itemsize for a in args) + out_shape.size * out_shape.dtype.itemsize
    return pl.pallas_call(
        body,
        out_shape=out_shape,
        grid_spec=pltpu.PrefetchScalarGridSpec(
            num_scalar_prefetch=len(tables), grid=(grid,), in_specs=in_specs,
            out_specs=out_spec, scratch_shapes=scratch,
        ),
        compiler_params=pltpu.CompilerParams(vmem_limit_bytes=62 * 1024 * 1024),
        cost_estimate=pl.CostEstimate(flops=flops, bytes_accessed=moved, transcendentals=0),
        name=name,
    )(*tables, *args)


class Tables:
    def __init__(self, slots, layers, blocks):
        self.tgt, self.id, self.valid = 0, slots, 2 * slots
        self.prev_tgt, self.prev_id = 3 * slots, 4 * slots
        self.last_tgt = 5 * slots
        self.last_id = self.last_tgt + layers + 1
        self.size = -(-(self.last_id + blocks + 1) // 128) * 128


def slot_tables(dec_list, layers, blocks, blocks_layer):
    slots = dec_list.shape[0]
    at = Tables(slots, layers, blocks)

    def body(d_ref, o_ref):
        def clear(i, c):
            o_ref[i] = 0
            return c

        lax.fori_loop(0, at.size, clear, 0)

        def one(k, c):
            s, t, b = d_ref[k, 0], d_ref[k, 1], d_ref[k, 2]
            listed = t >= 0
            group = jnp.where(listed, t, layers)
            ident = jnp.where(listed, s * blocks_layer + b, blocks)
            o_ref[at.tgt + k] = jnp.maximum(t, 0)
            o_ref[at.id + k] = jnp.where(listed, ident, 0)
            o_ref[at.valid + k] = jnp.where(listed, 1, 0)
            o_ref[at.prev_tgt + k] = o_ref[at.last_tgt + group]
            o_ref[at.last_tgt + group] = k + 1
            o_ref[at.prev_id + k] = o_ref[at.last_id + ident]
            o_ref[at.last_id + ident] = k + 1
            return c

        lax.fori_loop(0, slots, one, 0)

    return pl.pallas_call(
        body,
        out_shape=jax.ShapeDtypeStruct((at.size,), jnp.int32),
        in_specs=[pl.BlockSpec(memory_space=pltpu.SMEM)],
        out_specs=pl.BlockSpec(memory_space=pltpu.SMEM),
        name="slot_tables",
    )(dec_list)


def chunk_count(toks):
    return next(c for c in (4, 2, 1) if toks % (16 * c) == 0 or c == 1)


def decode_total(tables, lat, dec_weight, targets, scale, cid):
    blocks, w_count, toks, block = lat.shape
    slots, _, width = dec_weight.shape
    layers = targets.shape[0]
    n = lax.axis_size("lay")
    at = Tables(slots, layers, blocks)
    chunks = chunk_count(toks)
    ct = toks // chunks
    rows = w_count * ct
    cuts = next(c for c in (CUTS, 1) if width % (128 * c) == 0)
    part = width // cuts
    steps = layers * cuts
    pieces = chunks * steps
    per_step = -(-slots // steps)

    def body(tab, lat_ref, w_hbm, t_ref, e_ref, w_ref, sums, own, up_in, dn_in, up_out, dn_out,
             wsem, us, ur, ds, dr):
        l = lax.axis_index("lay")

        def weight(k):
            return pltpu.make_async_copy(w_hbm.at[k], w_ref.at[k], wsem.at[k])

        loop(0, slots, lambda k: weight(k).start())
        barrier = pltpu.get_barrier_semaphore()
        others(l, n, lambda j: signal(barrier, lay=j))
        sums[0] = jnp.zeros_like(sums[0])
        pl.semaphore_wait(barrier, n - 1)

        def slot(c, k):
            held = lat_ref[tab[at.id + k], :, pl.ds(pl.multiple_of(c * ct, ct), ct), :]
            made = jnp.dot(held.reshape(rows, block), w_ref[k], preferred_element_type=F32)
            sums[k + 1] = made + sums[tab[at.prev_tgt + k]]

        def emit(c):
            for t in range(layers):
                total = sums[tab[at.last_tgt + t]]
                for i in range(cuts):
                    own[(c * layers + t) * cuts + i] = total[:, i * part:(i + 1) * part]

        def first(k, c):
            weight(k).wait()
            slot(0, k)
            return c

        lax.fori_loop(0, slots, first, 0)
        emit(0)

        def up(q):
            return remote(up_out.at[q], up_in.at[q], us.at[q], ur.at[q], lay=l + 1)

        def dn(q):
            return remote(dn_out.at[q], dn_in.at[q], ds.at[q], dr.at[q], lay=l - 1)

        def landed_up(q):
            remote(up_in.at[q], up_in.at[q], us.at[q], ur.at[q], lay=l).wait_recv()

        def landed_dn(q):
            remote(dn_in.at[q], dn_in.at[q], ds.at[q], dr.at[q], lay=l).wait_recv()

        def inside(q):
            return (q >= 0) & (q < pieces)

        def hand_on(s):
            q, p = s - SKEW * l, s - SKEW * (n - 1 - l)

            @pl.when(inside(q) & (l > 0))
            def _():
                landed_up(q)

            @pl.when(inside(q) & (l == 0))
            def _():
                up_out[q] = own[q].astype(BF16)

            @pl.when(inside(q) & (l > 0) & (l < n - 1))
            def _():
                up_out[q] = (own[q] + up_in[q].astype(F32)).astype(BF16)

            @pl.when(inside(p) & (l < n - 1))
            def _():
                landed_dn(p)

            @pl.when(inside(p) & (l == n - 1))
            def _():
                dn_out[p] = own[p].astype(BF16)

            @pl.when(inside(p) & (l > 0) & (l < n - 1))
            def _():
                dn_out[p] = (own[p] + dn_in[p].astype(F32)).astype(BF16)

            e = s - SKEW * jnp.maximum(l, n - 1 - l)

            def error(total):
                c, i = e // steps, lax.rem(e, steps)
                t, i = i // cuts, lax.rem(i, cuts)
                where = pl.ds(pl.multiple_of(c * ct, ct), ct)
                over = pl.ds(pl.multiple_of(i * part, part), part)
                aim = t_ref[t, :, where, over].reshape(rows, part).astype(F32)
                e_ref[t, :, where, over] = ((total - aim) * scale).astype(BF16).reshape(w_count, ct, part)

            @pl.when(inside(e) & (l == 0))
            def _():
                error(own[e] + dn_in[e].astype(F32))

            @pl.when(inside(e) & (l == n - 1))
            def _():
                error(own[e] + up_in[e].astype(F32))

            @pl.when(inside(e) & (l > 0) & (l < n - 1))
            def _():
                error(own[e] + up_in[e].astype(F32) + dn_in[e].astype(F32))

            @pl.when(inside(q) & (l < n - 1))
            def _():
                up(q).start()

            @pl.when(inside(p) & (l > 0))
            def _():
                dn(p).start()

        def turn(s, carry):
            hand_on(s)
            c, i = s // steps + 1, lax.rem(s, steps)

            @pl.when(c < chunks)
            def _():
                for j in range(per_step):
                    @pl.when(i * per_step + j < slots)
                    def _():
                        slot(c, i * per_step + j)

                @pl.when(i == steps - 1)
                def _():
                    emit(c)

            return carry

        lax.fori_loop(0, pieces + SKEW * (n - 1), turn, 0)

        def sent(q, c):
            @pl.when(l < n - 1)
            def _():
                up(q).wait_send()

            @pl.when(l > 0)
            def _():
                dn(q).wait_send()

            return c

        lax.fori_loop(0, pieces, sent, 0)

    piece = (pieces, rows, part)
    vmem = pl.BlockSpec(memory_space=pltpu.VMEM)
    return pl.pallas_call(
        body,
        out_shape=jax.ShapeDtypeStruct((layers, w_count, toks, width), BF16),
        in_specs=[pl.BlockSpec(memory_space=pltpu.SMEM), vmem, ANY, vmem],
        out_specs=vmem,
        scratch_shapes=[
            pltpu.VMEM(dec_weight.shape, dec_weight.dtype),
            pltpu.VMEM((slots + 1, rows, width), F32),
            pltpu.VMEM(piece, F32),
        ] + [pltpu.VMEM(piece, BF16)] * 4 + [pltpu.SemaphoreType.DMA((slots,))]
        + [pltpu.SemaphoreType.DMA((pieces,))] * 4,
        compiler_params=pltpu.CompilerParams(
            collective_id=cid, has_side_effects=True, vmem_limit_bytes=62 * 1024 * 1024
        ),
        name="decode_total",
    )(tables, lat, dec_weight, targets)


def slot_errors(tgt, err, dec_weight):
    slots, block, width = dec_weight.shape
    layers, toks, _ = err.shape
    g = group_of(slots)

    def body(t_ref, e_ref, w_ref, o_ref):
        for i in range(g):
            k = pl.program_id(0) * g + i
            o_ref[i] = lax.dot_general(
                e_ref[t_ref[k]], w_ref[i], (((1,), (1,)), ((), ())), preferred_element_type=F32
            ).astype(o_ref.dtype)

    return slot_call(
        body, (tgt,), (err, dec_weight),
        [pl.BlockSpec((layers, toks, width), lambda k, t: (0, 0, 0)),
         pl.BlockSpec((g, block, width), lambda k, t: (k, 0, 0))],
        jax.ShapeDtypeStruct((slots, toks, block), BF16),
        pl.BlockSpec((g, toks, block), lambda k, t: (k, 0, 0)),
        [], 2 * slots * toks * block * width, "slot_errors", slots // g,
    )


def combine(ids, valid, parts, blocks_total):
    w_count, slots, toks, block = parts.shape

    g = slots // 3 if slots % 3 == 0 else 1

    def body(i_ref, v_ref, p_ref, o_ref, acc):
        step = pl.program_id(0)

        @pl.when(step == 0)
        def _():
            acc[...] = jnp.zeros_like(acc)

        for i in range(g):
            k = step * g + i

            @pl.when(v_ref[k] > 0)
            def _():
                acc[i_ref[k]] += jnp.sum(p_ref[:, i].astype(F32), axis=0)

        @pl.when(step == slots // g - 1)
        def _():
            o_ref[...] = acc[...].astype(o_ref.dtype)

    return slot_call(
        body, (ids, valid), (parts,),
        [pl.BlockSpec((w_count, g, toks, block), lambda k, i, v: (0, k, 0, 0))],
        jax.ShapeDtypeStruct((blocks_total, toks, block), BF16),
        pl.BlockSpec((blocks_total, toks, block), lambda k, i, v: (0, 0, 0)),
        [pltpu.VMEM((blocks_total, toks, block), F32)], w_count * slots * toks * block, "combine",
        slots // g,
    )


def decoder_grads(ids, tgt, valid, rep, lat, lat_twin, err, err_twin, slots):
    layers, toks, width = err.shape
    blocks, _, half = lat_twin.shape
    g = group_of(slots)

    def body(i_ref, t_ref, v_ref, r_ref, l_ref, lt_ref, e_ref, et_ref, o_ref):
        over = (((0,), (0,)), ((), ()))
        for i in range(g):
            k = pl.program_id(0) * g + i

            @pl.when(v_ref[k] > 0)
            def _():
                t, b = t_ref[k], i_ref[k]
                o_ref[i] = lax.dot_general(
                    l_ref[b], e_ref[t], over, preferred_element_type=F32
                ) + lax.dot_general(lt_ref[b], et_ref[t], over, preferred_element_type=F32)

            @pl.when(v_ref[k] == 0)
            def _():
                o_ref[i] = jnp.zeros_like(o_ref[i])

    return slot_call(
        body, (ids, tgt, valid, rep), (lat, lat_twin, err, err_twin),
        [pl.BlockSpec((blocks, toks, half), lambda k, i, t, v, r: (0, 0, r[0])),
         pl.BlockSpec((blocks, toks, half), lambda k, i, t, v, r: (0, 0, 0)),
         pl.BlockSpec((layers, toks, width), lambda k, i, t, v, r: (0, 0, 0)),
         pl.BlockSpec((layers, toks, width), lambda k, i, t, v, r: (0, 0, 0))],
        jax.ShapeDtypeStruct((slots, half, width), F32),
        pl.BlockSpec((g, half, width), lambda k, i, t, v, r: (k, 0, 0)),
        [], 4 * slots * toks * half * width, "decoder_grads", slots // g,
    )


def local(acts, targets, enc_weight, enc_bias, gate_mask, dec_list, dec_weight):
    layers, tok_rows, width_part = acts.shape
    lat_dev = enc_weight.shape[1]
    slots, block, _ = dec_weight.shape
    per_dev = lat_dev // block
    n, w_count, r_count = lax.axis_size("lay"), lax.axis_size("wid"), lax.axis_size("rep")
    lay, wid, rep = lax.axis_index("lay"), lax.axis_index("wid"), lax.axis_index("rep")
    lat_total = lat_dev * n
    blocks_total = lat_total // block
    latents_layer = lat_total // layers
    blocks_layer = latents_layer // block
    toks = tok_rows // w_count

    tgt = dec_list[:, 1]
    valid = (tgt >= 0).astype(jnp.int32)
    ids = jnp.maximum(dec_list[:, 0] * blocks_layer + dec_list[:, 2], 0)
    tgt = jnp.maximum(tgt, 0)

    here = lax.dynamic_index_in_dim(acts, lay * lat_dev // latents_layer, 0, keepdims=False)
    partial = jnp.dot(here, enc_weight, preferred_element_type=F32).astype(BF16)
    parts = exchange(
        "wid", partial.reshape(w_count, toks, lat_dev), (w_count, toks, lat_dev), (toks, lat_dev),
        lambda x, j: x.at[j], lambda o, j: o.at[j], 0,
    )
    shifted = jnp.sum(parts.astype(F32), axis=0) + enc_bias[None, :]
    shifted = shifted.reshape(toks, per_dev, block).transpose(1, 0, 2)
    keep = lax.dynamic_slice_in_dim(gate_mask, wid * toks, toks, 0).astype(F32).T[:, :, None]
    latent = (smooth_gate(shifted) * keep).astype(BF16)
    lat = gather_latents(latent, 1)

    scale = float(tok_rows * r_count) ** (-0.5)
    err = decode_total(
        slot_tables(dec_list, layers, blocks_total, blocks_layer), lat, dec_weight,
        targets.reshape(layers, w_count, toks, width_part), scale, 2,
    ).reshape(layers, tok_rows, width_part)
    lat = lat.reshape(blocks_total, tok_rows, block)

    slot_err = slot_errors(tgt, err, dec_weight).reshape(slots, w_count, toks, block)
    slot_in, lat_twin, err_twin, acts_all = slots_and_twin(slot_err, lat, err, here, 4)
    outgoing = combine(ids, valid, slot_in, blocks_total)
    outgoing = outgoing.reshape(n, per_dev, toks, block)
    incoming = [lax.dynamic_index_in_dim(outgoing, lay, 0, keepdims=False)]
    for d in range(1, n):
        part = lax.dynamic_index_in_dim(outgoing, lax.rem(lay + d, n), 0, keepdims=False)
        incoming.append(lax.ppermute(part, "lay", [(i, (i + d) % n) for i in range(n)]))
    dec_out = decoder_grads(
        ids, tgt, valid, rep.reshape(1).astype(jnp.int32), lat, lat_twin, err, err_twin, slots
    )
    latent_error = sum(part.astype(F32) for part in incoming)
    pre_grad = (latent_error * keep * gate_slope(shifted)).astype(BF16)
    columns = lat_dev // r_count
    pre_grad = pre_grad.transpose(1, 0, 2).reshape(toks, r_count, columns).transpose(1, 0, 2)
    pre_all = gather_pre_grad(pre_grad, 6).reshape(r_count, tok_rows, columns)

    enc_out = lax.dot_general(
        acts_all.reshape(r_count * tok_rows, width_part),
        pre_all.reshape(r_count * tok_rows, columns), (((0,), (0,)), ((), ())),
        preferred_element_type=F32,
    )
    bias_out = jnp.sum(pre_all.astype(F32), axis=(0, 1))
    return (enc_out, bias_out, dec_out)


def solution(mesh):
    return jax.shard_map(
        local,
        mesh=mesh,
        in_specs=(
            P(None, ("grp", "rep"), "wid"),
            P(None, ("grp", "rep"), "wid"),
            P("wid", "lay"),
            P("lay"),
            P(("grp", "rep"), "lay"),
            P("lay", None),
            P("lay", None, "wid"),
        ),
        out_specs=(
            P(("grp", "wid"), ("lay", "rep")),
            P(("grp", "lay", "rep")),
            P(("grp", "lay"), "rep", "wid"),
        ),
        check_vma=False,
    )
```

```python
import jax
import jax.numpy as jnp
from jax import lax
from jax.experimental import pallas as pl
from jax.experimental.pallas import tpu as pltpu
from jax.sharding import PartitionSpec as P

ROOT = 0.7978845608028654
CUBIC = 0.044715
MESH = pl.DeviceIdType.MESH
BF16 = jnp.bfloat16
F32 = jnp.float32
CUTS = 2
SKEW = 3
Z_SKEW = 3


def smooth_gate(shifted):
    inside_arg = ROOT * (shifted + CUBIC * shifted * shifted * shifted)
    return 0.5 * shifted * (1.0 + jnp.tanh(inside_arg))


def gate_slope(shifted):
    inside_arg = ROOT * (shifted + CUBIC * shifted * shifted * shifted)
    tanh_part = jnp.tanh(inside_arg)
    return 0.5 * (1.0 + tanh_part) + 0.5 * shifted * (1.0 - tanh_part * tanh_part) * ROOT * (
        1.0 + 3.0 * CUBIC * shifted * shifted
    )


def loop(first, count, step):
    if count <= 4:
        for d in range(first, count):
            step(d)
    else:
        lax.fori_loop(first, count, lambda d, c: (step(d), c)[1], 0)


def others(me, count, step):
    loop(1, count, lambda d: step(lax.rem(me + d, count)))


def signal(barrier, **where):
    pl.semaphore_signal(barrier, inc=1, device_id=where, device_id_type=MESH)


def remote(src, dst, send_sem, recv_sem, **where):
    return pltpu.make_async_remote_copy(
        src_ref=src, dst_ref=dst, send_sem=send_sem, recv_sem=recv_sem, device_id=where,
        device_id_type=MESH,
    )


ANY = pl.BlockSpec(memory_space=pl.ANY)


def bounce(src, dst, held, sem):
    into = pltpu.make_async_copy(src, held, sem)
    into.start()
    into.wait()
    out = pltpu.make_async_copy(held, dst, sem)
    out.start()
    return out


def nearest(l, n, step):
    def both(d):
        for j in (l - d, l + d):

            @pl.when((j >= 0) & (j < n))
            def _():
                step(j)

    loop(1, n, both)


def line_gather(l, n, src, slot, send_sem, recv_sem, arrived):
    def own(step):
        @pl.when(l < n - 1)
        def _():
            step(remote(src, slot(l), send_sem.at[l], recv_sem.at[l], lay=l + 1))

        @pl.when(l > 0)
        def _():
            step(remote(src, slot(l), send_sem.at[n], recv_sem.at[l], lay=l - 1))

    def hop(j, step):
        @pl.when((j < l) & (l < n - 1))
        def _():
            step(remote(slot(j), slot(j), send_sem.at[j], recv_sem.at[j], lay=l + 1))

        @pl.when((j > l) & (l > 0))
        def _():
            step(remote(slot(j), slot(j), send_sem.at[j], recv_sem.at[j], lay=l - 1))

    def take(j):
        remote(slot(j), slot(j), send_sem.at[j], recv_sem.at[j], lay=j).wait_recv()
        hop(j, lambda c: c.start())
        arrived(j)

    def finish():
        own(lambda c: c.wait_send())
        nearest(l, n, lambda j: hop(j, lambda c: c.wait_send()))

    own(lambda c: c.start())
    return lambda: nearest(l, n, take), finish


def comm(body, args, outs, sems, cid, held=()):
    return pl.pallas_call(
        body,
        out_shape=tuple(outs),
        in_specs=[ANY] * len(args),
        out_specs=tuple([ANY] * len(outs)),
        scratch_shapes=[pltpu.SemaphoreType.DMA((s,)) for s in sems] + [pltpu.VMEM(*h) for h in held],
        compiler_params=pltpu.CompilerParams(collective_id=cid, has_side_effects=True),
        name=f"exchange_{cid}",
    )(*args)


def exchange(axis, x, out_shape, held_shape, src_of, dst_of, cid):
    n = lax.axis_size(axis)

    def body(x_ref, o_ref, ssem, rsem, lsem, held):
        me = lax.axis_index(axis)
        barrier = pltpu.get_barrier_semaphore()
        others(me, n, lambda j: signal(barrier, **{axis: j}))
        pl.semaphore_wait(barrier, n - 1)

        def send(j):
            return remote(
                src_of(x_ref, j), dst_of(o_ref, me), ssem.at[j], rsem.at[me], **{axis: j}
            )

        def arrival(j):
            return remote(
                src_of(x_ref, me), dst_of(o_ref, j), ssem.at[j], rsem.at[j], **{axis: j}
            )

        others(me, n, lambda j: send(j).start())
        own = bounce(src_of(x_ref, me), dst_of(o_ref, me), held, lsem.at[0])
        others(me, n, lambda j: arrival(j).wait_recv())
        others(me, n, lambda j: send(j).wait_send())
        own.wait()

    return comm(
        body, [x], [jax.ShapeDtypeStruct(out_shape, x.dtype)], (n, n, 1), cid,
        [(held_shape, x.dtype)],
    )[0]


def gather_latents(h, cid):
    n, w_count = lax.axis_size("lay"), lax.axis_size("wid")
    blocks, toks, width = h.shape

    def body(h_ref, o_ref, zs, zr, xs, xr, lsem, held):
        l, w = lax.axis_index("lay"), lax.axis_index("wid")
        barrier = pltpu.get_barrier_semaphore()
        others(l, n, lambda j: signal(barrier, lay=j))
        others(w, w_count, lambda v: signal(barrier, wid=v))
        pl.semaphore_wait(barrier, n + w_count - 2)

        def slot(j, v):
            return o_ref.at[pl.ds(j * blocks, blocks), v]

        def x_own(v):
            return remote(h_ref, slot(l, w), xs.at[l * w_count + v], xr.at[l * w_count + w], wid=v)

        def x_copy(j, v, source):
            return remote(
                slot(j, source), slot(j, source), xs.at[j * w_count + v],
                xr.at[j * w_count + source], wid=v,
            )

        take, finish = line_gather(
            l, n, h_ref, lambda j: slot(j, w), zs, zr,
            lambda j: others(w, w_count, lambda v: x_copy(j, v, w).start()),
        )
        others(w, w_count, lambda v: x_own(v).start())
        own = bounce(h_ref, slot(l, w), held, lsem.at[0])
        take()
        finish()
        others(w, w_count, lambda v: x_own(v).wait_send())
        nearest(l, n, lambda j: others(w, w_count, lambda v: x_copy(j, v, w).wait_send()))
        loop(0, n, lambda j: others(w, w_count, lambda v: x_copy(j, v, v).wait_recv()))
        own.wait()

    out = jax.ShapeDtypeStruct((n * blocks, w_count, toks, width), h.dtype)
    return comm(
        body, [h], [out], (n + 1, n, n * w_count, n * w_count, 1), cid, [(h.shape, h.dtype)]
    )[0]


def group_of(slots):
    return 3 if slots % 3 == 0 else 1


def slot_call(body, tables, args, in_specs, out_shape, out_spec, scratch, flops, name, grid):
    moved = sum(a.size * a.dtype.itemsize for a in args) + out_shape.size * out_shape.dtype.itemsize
    return pl.pallas_call(
        body,
        out_shape=out_shape,
        grid_spec=pltpu.PrefetchScalarGridSpec(
            num_scalar_prefetch=len(tables), grid=(grid,), in_specs=in_specs,
            out_specs=out_spec, scratch_shapes=scratch,
        ),
        compiler_params=pltpu.CompilerParams(vmem_limit_bytes=62 * 1024 * 1024),
        cost_estimate=pl.CostEstimate(flops=flops, bytes_accessed=moved, transcendentals=0),
        name=name,
    )(*tables, *args)


class Tables:
    def __init__(self, slots, layers, blocks):
        self.tgt, self.id, self.valid = 0, slots, 2 * slots
        self.prev_tgt, self.prev_id = 3 * slots, 4 * slots
        self.last_tgt = 5 * slots
        self.last_id = self.last_tgt + layers + 1
        self.size = -(-(self.last_id + blocks + 1) // 128) * 128


def slot_tables(dec_list, layers, blocks, blocks_layer):
    slots = dec_list.shape[0]
    at = Tables(slots, layers, blocks)

    def body(d_ref, o_ref):
        def clear(i, c):
            o_ref[i] = 0
            return c

        lax.fori_loop(0, at.size, clear, 0)

        def one(k, c):
            s, t, b = d_ref[k, 0], d_ref[k, 1], d_ref[k, 2]
            listed = t >= 0
            group = jnp.where(listed, t, layers)
            ident = jnp.where(listed, s * blocks_layer + b, blocks)
            o_ref[at.tgt + k] = jnp.maximum(t, 0)
            o_ref[at.id + k] = jnp.where(listed, ident, 0)
            o_ref[at.valid + k] = jnp.where(listed, 1, 0)
            o_ref[at.prev_tgt + k] = o_ref[at.last_tgt + group]
            o_ref[at.last_tgt + group] = k + 1
            o_ref[at.prev_id + k] = o_ref[at.last_id + ident]
            o_ref[at.last_id + ident] = k + 1
            return c

        lax.fori_loop(0, slots, one, 0)

    return pl.pallas_call(
        body,
        out_shape=jax.ShapeDtypeStruct((at.size,), jnp.int32),
        in_specs=[pl.BlockSpec(memory_space=pltpu.SMEM)],
        out_specs=pl.BlockSpec(memory_space=pltpu.SMEM),
        name="slot_tables",
    )(dec_list)


def chunk_count(toks):
    return next(c for c in (4, 2, 1) if toks % (16 * c) == 0 or c == 1)


def decode_total(tables, lat, dec_weight, targets, scale, cid):
    blocks, w_count, toks, block = lat.shape
    slots, _, width = dec_weight.shape
    layers = targets.shape[0]
    n = lax.axis_size("lay")
    at = Tables(slots, layers, blocks)
    chunks = chunk_count(toks)
    ct = toks // chunks
    rows = w_count * ct
    cuts = next(c for c in (CUTS, 1) if width % (128 * c) == 0)
    part = width // cuts
    steps = layers * cuts
    pieces = chunks * steps
    per_step = -(-slots // steps)

    def body(tab, lat_ref, w_hbm, t_ref, e_ref, w_ref, sums, own, up_in, dn_in, up_out, dn_out,
             wsem, us, ur, ds, dr):
        l = lax.axis_index("lay")

        def weight(k):
            return pltpu.make_async_copy(w_hbm.at[k], w_ref.at[k], wsem.at[k])

        loop(0, slots, lambda k: weight(k).start())
        barrier = pltpu.get_barrier_semaphore()
        others(l, n, lambda j: signal(barrier, lay=j))
        sums[0] = jnp.zeros_like(sums[0])
        pl.semaphore_wait(barrier, n - 1)

        def slot(c, k):
            held = lat_ref[tab[at.id + k], :, pl.ds(pl.multiple_of(c * ct, ct), ct), :]
            made = jnp.dot(held.reshape(rows, block), w_ref[k], preferred_element_type=F32)
            sums[k + 1] = made + sums[tab[at.prev_tgt + k]]

        def emit(c):
            for t in range(layers):
                total = sums[tab[at.last_tgt + t]]
                for i in range(cuts):
                    own[(c * layers + t) * cuts + i] = total[:, i * part:(i + 1) * part]

        def first(k, c):
            weight(k).wait()
            slot(0, k)
            return c

        lax.fori_loop(0, slots, first, 0)
        emit(0)

        def up(q):
            return remote(up_out.at[q], up_in.at[q], us.at[q], ur.at[q], lay=l + 1)

        def dn(q):
            return remote(dn_out.at[q], dn_in.at[q], ds.at[q], dr.at[q], lay=l - 1)

        def landed_up(q):
            remote(up_in.at[q], up_in.at[q], us.at[q], ur.at[q], lay=l).wait_recv()

        def landed_dn(q):
            remote(dn_in.at[q], dn_in.at[q], ds.at[q], dr.at[q], lay=l).wait_recv()

        def inside(q):
            return (q >= 0) & (q < pieces)

        def hand_on(s):
            q, p = s - SKEW * l, s - SKEW * (n - 1 - l)

            @pl.when(inside(q) & (l > 0))
            def _():
                landed_up(q)

            @pl.when(inside(q) & (l == 0))
            def _():
                up_out[q] = own[q].astype(BF16)

            @pl.when(inside(q) & (l > 0) & (l < n - 1))
            def _():
                up_out[q] = (own[q] + up_in[q].astype(F32)).astype(BF16)

            @pl.when(inside(p) & (l < n - 1))
            def _():
                landed_dn(p)

            @pl.when(inside(p) & (l == n - 1))
            def _():
                dn_out[p] = own[p].astype(BF16)

            @pl.when(inside(p) & (l > 0) & (l < n - 1))
            def _():
                dn_out[p] = (own[p] + dn_in[p].astype(F32)).astype(BF16)

            e = s - SKEW * jnp.maximum(l, n - 1 - l)

            def error(total):
                c, i = e // steps, lax.rem(e, steps)
                t, i = i // cuts, lax.rem(i, cuts)
                where = pl.ds(pl.multiple_of(c * ct, ct), ct)
                over = pl.ds(pl.multiple_of(i * part, part), part)
                aim = t_ref[t, :, where, over].reshape(rows, part).astype(F32)
                e_ref[t, :, where, over] = ((total - aim) * scale).astype(BF16).reshape(w_count, ct, part)

            @pl.when(inside(e) & (l == 0))
            def _():
                error(own[e] + dn_in[e].astype(F32))

            @pl.when(inside(e) & (l == n - 1))
            def _():
                error(own[e] + up_in[e].astype(F32))

            @pl.when(inside(e) & (l > 0) & (l < n - 1))
            def _():
                error(own[e] + up_in[e].astype(F32) + dn_in[e].astype(F32))

            @pl.when(inside(q) & (l < n - 1))
            def _():
                up(q).start()

            @pl.when(inside(p) & (l > 0))
            def _():
                dn(p).start()

        def turn(s, carry):
            hand_on(s)
            c, i = s // steps + 1, lax.rem(s, steps)

            @pl.when(c < chunks)
            def _():
                for j in range(per_step):
                    @pl.when(i * per_step + j < slots)
                    def _():
                        slot(c, i * per_step + j)

                @pl.when(i == steps - 1)
                def _():
                    emit(c)

            return carry

        lax.fori_loop(0, pieces + SKEW * (n - 1), turn, 0)

        def sent(q, c):
            @pl.when(l < n - 1)
            def _():
                up(q).wait_send()

            @pl.when(l > 0)
            def _():
                dn(q).wait_send()

            return c

        lax.fori_loop(0, pieces, sent, 0)

    piece = (pieces, rows, part)
    vmem = pl.BlockSpec(memory_space=pltpu.VMEM)
    return pl.pallas_call(
        body,
        out_shape=jax.ShapeDtypeStruct((layers, w_count, toks, width), BF16),
        in_specs=[pl.BlockSpec(memory_space=pltpu.SMEM), vmem, ANY, vmem],
        out_specs=vmem,
        scratch_shapes=[
            pltpu.VMEM(dec_weight.shape, dec_weight.dtype),
            pltpu.VMEM((slots + 1, rows, width), F32),
            pltpu.VMEM(piece, F32),
        ] + [pltpu.VMEM(piece, BF16)] * 4 + [pltpu.SemaphoreType.DMA((slots,))]
        + [pltpu.SemaphoreType.DMA((pieces,))] * 4,
        compiler_params=pltpu.CompilerParams(
            collective_id=cid, has_side_effects=True, vmem_limit_bytes=62 * 1024 * 1024
        ),
        name="decode_total",
    )(tables, lat, dec_weight, targets)


def latent_errors(tables, err, dec_weight, slope, lat, acts_here, cid):
    layers, w_count, toks, width = err.shape
    slots, block, _ = dec_weight.shape
    per_dev = slope.shape[0]
    n, r_count = lax.axis_size("lay"), lax.axis_size("rep")
    assert r_count == 2
    blocks = lat.shape[0]
    columns = per_dev * block // r_count
    at = Tables(slots, layers, blocks)
    chunks = chunk_count(toks)
    ct = toks // chunks
    rows = w_count * ct
    split = 2 if per_dev % 2 == 0 else 1
    pb = per_dev // split
    steps = (n - 1) * split
    pieces = chunks * steps
    g = group_of(slots)
    groups = slots // g
    lead = min(2, chunks)
    half = block // r_count

    def body(tab, e_ref, w_hbm, sl_ref, l_ref, a_ref, po_ref, lo_ref, eo_ref, ao_ref,
             w_ref, x_out, x_in, sums, made, up_in, dn_in, up_out, dn_out, twin_out,
             wsem, xs, xr, us, ur, ds, dr, ts, tr, ps, pr, asem):
        l, w, r = lax.axis_index("lay"), lax.axis_index("wid"), lax.axis_index("rep")
        twin = 1 - r

        def weight(k):
            return pltpu.make_async_copy(w_hbm.at[k], w_ref.at[k], wsem.at[k])

        loop(0, slots, lambda k: weight(k).start())
        barrier = pltpu.get_barrier_semaphore()
        others(l, n, lambda j: signal(barrier, lay=j))
        others(w, w_count, lambda v: signal(barrier, wid=v))
        signal(barrier, rep=twin)
        sums[0] = jnp.zeros_like(sums[0])
        pl.semaphore_wait(barrier, n + w_count - 1)

        def chunk(c):
            return pl.ds(pl.multiple_of(c * ct, ct), ct)

        def x_send(c, i, v):
            where = pl.ds(i * g, g)
            return remote(x_out.at[c, v, where], x_in.at[c, w, where], xs.at[(c * groups + i) * w_count + v],
                          xr.at[(c * groups + i) * w_count + w], wid=v)

        def x_landed(c, i, v):
            where = pl.ds(i * g, g)
            return remote(x_in.at[c, v, where], x_in.at[c, v, where],
                          xs.at[(c * groups + i) * w_count + v],
                          xr.at[(c * groups + i) * w_count + v], wid=v)

        def slot_group(c, i, fresh=False):
            for k in [i * g + d for d in range(g)]:
                if fresh:
                    weight(k).wait()
                held = e_ref[tab[at.tgt + k], :, chunk(c), :].reshape(rows, width)
                part = lax.dot_general(
                    held, w_ref[k], (((1,), (1,)), ((), ())), preferred_element_type=F32
                ).astype(BF16).reshape(w_count, ct, block)
                for v in range(w_count):
                    x_out[c, v, k] = part[v]
            others(w, w_count, lambda v: x_send(c, i, v).start())

        twins = [
            remote(l_ref.at[:, :, :, pl.ds(pl.multiple_of(twin * half, half), half)], lo_ref,
                   ts.at[0], tr.at[0], rep=twin),
            remote(e_ref, eo_ref, ts.at[1], tr.at[1], rep=twin),
        ] + [
            remote(a_ref.at[v], ao_ref.at[lax.rem(v - w + w_count, w_count), r], ts.at[2 + v], tr.at[2 + v],
                   rep=twin)
            for v in range(w_count)
        ]
        mine = [
            pltpu.make_async_copy(
                a_ref.at[v], ao_ref.at[lax.rem(v - w + w_count, w_count), r], asem.at[v])
            for v in range(w_count)
        ]

        def gather(c):
            def landed(i, carry):
                others(w, w_count, lambda v: x_landed(c, i, v).wait_recv())
                return carry

            lax.fori_loop(0, groups, landed, 0)

            def one(k, carry):
                total = sums[tab[at.prev_id + k]] + x_out[c, w, k].astype(F32)
                for d in range(1, w_count):
                    total = total + x_in[c, lax.rem(w + d, w_count), k].astype(F32)
                sums[k + 1] = total
                return carry

            lax.fori_loop(0, slots, one, 0)

            def out(b, carry):
                made[c, b] = sums[tab[at.last_id + b]]
                return carry

            lax.fori_loop(0, blocks, out, 0)

        lax.fori_loop(0, groups, lambda i, z: (slot_group(0, i, True), z)[1], 0)
        for c in range(1, lead):
            lax.fori_loop(0, groups, lambda i, z: (slot_group(c, i), z)[1], 0)
        for c in twins + mine:
            c.start()
        gather(0)

        def up(q):
            return remote(up_out.at[q], up_in.at[q], us.at[q], ur.at[q], lay=l + 1)

        def dn(q):
            return remote(dn_out.at[q], dn_in.at[q], ds.at[q], dr.at[q], lay=l - 1)

        def landed_up(q):
            remote(up_in.at[q], up_in.at[q], us.at[q], ur.at[q], lay=l).wait_recv()

        def landed_dn(q):
            remote(dn_in.at[q], dn_in.at[q], ds.at[q], dr.at[q], lay=l).wait_recv()

        def inside(q):
            return (q >= 0) & (q < pieces)

        def own(q, dest):
            return made[q // steps, pl.ds(dest * per_dev + lax.rem(q, split) * pb, pb)]

        def tick(s, carry):
            q, p = s - Z_SKEW * l, s - Z_SKEW * (n - 1 - l)
            to_up = n - 1 - lax.rem(q + steps, steps) // split
            to_dn = lax.rem(p + steps, steps) // split

            @pl.when(inside(q) & (l > 0) & (to_up >= l))
            def _():
                landed_up(q)

            @pl.when(inside(q) & (l == 0))
            def _():
                up_out[q] = own(q, to_up).astype(BF16)

            @pl.when(inside(q) & (l > 0) & (to_up > l))
            def _():
                up_out[q] = (own(q, to_up) + up_in[q].astype(F32)).astype(BF16)

            @pl.when(inside(p) & (l < n - 1) & (to_dn <= l))
            def _():
                landed_dn(p)

            @pl.when(inside(p) & (l == n - 1))
            def _():
                dn_out[p] = own(p, to_dn).astype(BF16)

            @pl.when(inside(p) & (l < n - 1) & (to_dn < l))
            def _():
                dn_out[p] = (own(p, to_dn) + dn_in[p].astype(F32)).astype(BF16)

            off_up = (n - 1 - l) * split
            off_dn = l * split
            f = s - jnp.maximum(off_up + Z_SKEW * l, off_dn + Z_SKEW * (n - 1 - l))
            c, i = f // steps, lax.rem(f + steps, steps)
            whole = inside(f) & (i < split)

            def finish(total):
                blocks_here = pl.ds(i * pb, pb)
                grad = (total * sl_ref[blocks_here, chunk(c), :]).astype(BF16)
                if split == r_count:
                    @pl.when(i == r)
                    def _():
                        for b in range(pb):
                            po_ref[r, chunk(c), b * block:(b + 1) * block] = grad[b]

                    @pl.when(i != r)
                    def _():
                        for b in range(pb):
                            twin_out[c, :, b * block:(b + 1) * block] = grad[b]
                else:
                    for b in range(pb):
                        for side in range(r_count):
                            part = grad[b][:, side * half:(side + 1) * half]

                            @pl.when(r == side)
                            def _():
                                po_ref[side, chunk(c), b * half:(b + 1) * half] = part

                            @pl.when(r != side)
                            def _():
                                twin_out[c, :, b * half:(b + 1) * half] = part

            def mid():
                return made[c, pl.ds(l * per_dev + i * pb, pb)]

            @pl.when(whole & (l == 0))
            def _():
                finish(mid() + dn_in[c * steps + off_dn + i].astype(F32))

            @pl.when(whole & (l == n - 1))
            def _():
                finish(mid() + up_in[c * steps + off_up + i].astype(F32))

            @pl.when(whole & (l > 0) & (l < n - 1))
            def _():
                finish(mid() + up_in[c * steps + off_up + i].astype(F32)
                       + dn_in[c * steps + off_dn + i].astype(F32))

            @pl.when(inside(q) & (to_up > l))
            def _():
                up(q).start()

            @pl.when(inside(p) & (to_dn < l))
            def _():
                dn(p).start()

            @pl.when(whole & (i == split - 1))
            def _():
                twin_pre(c).start()

            c, i = s // steps, lax.rem(s, steps)

            @pl.when(c + lead < chunks)
            def _():
                lax.fori_loop(
                    (i * groups + steps - 1) // steps, ((i + 1) * groups + steps - 1) // steps,
                    lambda j, z: (slot_group(c + lead, j), z)[1], 0,
                )

            @pl.when((c + 1 < chunks) & (i == steps - 1))
            def _():
                gather(c + 1)

            return carry

        def twin_pre(c):
            return remote(twin_out.at[c], po_ref.at[r, chunk(c)], ps.at[c], pr.at[c], rep=twin)

        def twin_landed(c):
            return remote(twin_out.at[c], po_ref.at[twin, chunk(c)], ps.at[c], pr.at[c], rep=twin)

        lax.fori_loop(0, (chunks - 1) * steps + split + (n - 1) * max(split, Z_SKEW), tick, 0)

        def sent(q, carry):
            to_up = n - 1 - lax.rem(q, steps) // split
            to_dn = lax.rem(q, steps) // split

            @pl.when(to_up > l)
            def _():
                up(q).wait_send()

            @pl.when(to_dn < l)
            def _():
                dn(q).wait_send()

            return carry

        lax.fori_loop(0, pieces, sent, 0)

        def x_sent(q, carry):
            others(w, w_count, lambda v: x_send(q // groups, lax.rem(q, groups), v).wait_send())
            return carry

        lax.fori_loop(0, chunks * groups, x_sent, 0)
        for c in range(chunks):
            twin_landed(c).wait()
        for c in twins:
            c.wait()
        for c in mine:
            c.wait()

    piece = (pieces, pb, ct, block)
    x_shape = (chunks, w_count, slots, ct, block)
    vmem = pl.BlockSpec(memory_space=pltpu.VMEM)
    x_sems = chunks * groups * w_count
    dma = pltpu.SemaphoreType.DMA
    return pl.pallas_call(
        body,
        out_shape=(
            jax.ShapeDtypeStruct((r_count, toks, columns), BF16),
            jax.ShapeDtypeStruct(lat.shape[:3] + (half,), lat.dtype),
            jax.ShapeDtypeStruct(err.shape, err.dtype),
            jax.ShapeDtypeStruct((w_count, r_count, toks, width), acts_here.dtype),
        ),
        in_specs=[pl.BlockSpec(memory_space=pltpu.SMEM), vmem, ANY, vmem, ANY, vmem],
        out_specs=(vmem, ANY, ANY, ANY),
        scratch_shapes=[
            pltpu.VMEM(dec_weight.shape, dec_weight.dtype),
            pltpu.VMEM(x_shape, BF16),
            pltpu.VMEM(x_shape, BF16),
            pltpu.VMEM((slots + 1, ct, block), F32),
            pltpu.VMEM((chunks, blocks, ct, block), F32),
        ] + [pltpu.VMEM(piece, BF16)] * 4 + [
            pltpu.VMEM((chunks, ct, columns), BF16),
            dma((slots,)), dma((x_sems,)), dma((x_sems,)),
        ] + [dma((pieces,))] * 4 + [
            dma((2 + w_count,)), dma((2 + w_count,)), dma((chunks,)), dma((chunks,)), dma((w_count,)),
        ],
        compiler_params=pltpu.CompilerParams(
            collective_id=cid, has_side_effects=True, vmem_limit_bytes=62 * 1024 * 1024
        ),
        name="latent_errors",
    )(tables, err, dec_weight, slope, lat, acts_here)


def decoder_grads(ids, tgt, valid, rep, lat, lat_twin, err, err_twin, slots):
    layers, toks, width = err.shape
    blocks, _, half = lat_twin.shape
    g = group_of(slots)

    def body(i_ref, t_ref, v_ref, r_ref, l_ref, lt_ref, e_ref, et_ref, o_ref):
        over = (((0,), (0,)), ((), ()))
        for i in range(g):
            k = pl.program_id(0) * g + i

            @pl.when(v_ref[k] > 0)
            def _():
                t, b = t_ref[k], i_ref[k]
                o_ref[i] = lax.dot_general(
                    l_ref[b], e_ref[t], over, preferred_element_type=F32
                ) + lax.dot_general(lt_ref[b], et_ref[t], over, preferred_element_type=F32)

            @pl.when(v_ref[k] == 0)
            def _():
                o_ref[i] = jnp.zeros_like(o_ref[i])

    return slot_call(
        body, (ids, tgt, valid, rep), (lat, lat_twin, err, err_twin),
        [pl.BlockSpec((blocks, toks, half), lambda k, i, t, v, r: (0, 0, r[0])),
         pl.BlockSpec((blocks, toks, half), lambda k, i, t, v, r: (0, 0, 0)),
         pl.BlockSpec((layers, toks, width), lambda k, i, t, v, r: (0, 0, 0)),
         pl.BlockSpec((layers, toks, width), lambda k, i, t, v, r: (0, 0, 0))],
        jax.ShapeDtypeStruct((slots, half, width), F32),
        pl.BlockSpec((g, half, width), lambda k, i, t, v, r: (k, 0, 0)),
        [], 4 * slots * toks * half * width, "decoder_grads", slots // g,
    )


def local(acts, targets, enc_weight, enc_bias, gate_mask, dec_list, dec_weight):
    layers, tok_rows, width_part = acts.shape
    lat_dev = enc_weight.shape[1]
    slots, block, _ = dec_weight.shape
    per_dev = lat_dev // block
    n, w_count, r_count = lax.axis_size("lay"), lax.axis_size("wid"), lax.axis_size("rep")
    lay, wid, rep = lax.axis_index("lay"), lax.axis_index("wid"), lax.axis_index("rep")
    lat_total = lat_dev * n
    blocks_total = lat_total // block
    latents_layer = lat_total // layers
    blocks_layer = latents_layer // block
    toks = tok_rows // w_count

    tgt = dec_list[:, 1]
    valid = (tgt >= 0).astype(jnp.int32)
    ids = jnp.maximum(dec_list[:, 0] * blocks_layer + dec_list[:, 2], 0)
    tgt = jnp.maximum(tgt, 0)

    here = lax.dynamic_index_in_dim(acts, lay * lat_dev // latents_layer, 0, keepdims=False)
    partial = jnp.dot(here, enc_weight, preferred_element_type=F32).astype(BF16)
    parts = exchange(
        "wid", partial.reshape(w_count, toks, lat_dev), (w_count, toks, lat_dev), (toks, lat_dev),
        lambda x, j: x.at[j], lambda o, j: o.at[j], 0,
    )
    shifted = jnp.sum(parts.astype(F32), axis=0) + enc_bias[None, :]
    shifted = shifted.reshape(toks, per_dev, block).transpose(1, 0, 2)
    keep = lax.dynamic_slice_in_dim(gate_mask, wid * toks, toks, 0).astype(F32).T[:, :, None]
    latent = (smooth_gate(shifted) * keep).astype(BF16)
    lat = gather_latents(latent, 1)

    scale = float(tok_rows * r_count) ** (-0.5)
    tables = slot_tables(dec_list, layers, blocks_total, blocks_layer)
    err = decode_total(
        tables, lat, dec_weight, targets.reshape(layers, w_count, toks, width_part), scale, 2
    )
    slope = gate_slope(shifted) * keep
    pre_mine, lat_twin, err_twin, acts_all = latent_errors(
        tables, err, dec_weight, slope, lat, here.reshape(w_count, toks, width_part), 3
    )
    pre_all = [pre_mine] + [
        lax.ppermute(pre_mine, "wid", [(i, (i - d) % w_count) for i in range(w_count)])
        for d in range(1, w_count)
    ]
    half = block // r_count
    dec_out = decoder_grads(
        ids, tgt, valid, rep.reshape(1).astype(jnp.int32),
        lat.reshape(blocks_total, tok_rows, block), lat_twin.reshape(blocks_total, tok_rows, half),
        err.reshape(layers, tok_rows, width_part), err_twin.reshape(layers, tok_rows, width_part), slots,
    )
    columns = lat_dev // r_count
    pre_all = jnp.stack(pre_all).reshape(r_count * tok_rows, columns)
    enc_out = lax.dot_general(
        acts_all.reshape(r_count * tok_rows, width_part), pre_all, (((0,), (0,)), ((), ())),
        preferred_element_type=F32,
    )
    bias_out = jnp.sum(pre_all.astype(F32), axis=0)
    return (enc_out, bias_out, dec_out)


def solution(mesh):
    return jax.shard_map(
        local,
        mesh=mesh,
        in_specs=(
            P(None, ("grp", "rep"), "wid"),
            P(None, ("grp", "rep"), "wid"),
            P("wid", "lay"),
            P("lay"),
            P(("grp", "rep"), "lay"),
            P("lay", None),
            P("lay", None, "wid"),
        ),
        out_specs=(
            P(("grp", "wid"), ("lay", "rep")),
            P(("grp", "lay", "rep")),
            P(("grp", "lay"), "rep", "wid"),
        ),
        check_vma=False,
    )
```

```python
import jax
import jax.numpy as jnp
from jax import lax
from jax.experimental import pallas as pl
from jax.experimental.pallas import tpu as pltpu
from jax.sharding import PartitionSpec as P

ROOT = 0.7978845608028654
CUBIC = 0.044715
MESH = pl.DeviceIdType.MESH
BF16 = jnp.bfloat16
F32 = jnp.float32
CUTS = 2
SKEW = 3
Z_SKEW = 3
A_GATE = 3
A_SKEW = 3
A_ACROSS = 3
C_ACROSS = 3


def smooth_gate(shifted):
    inside_arg = ROOT * (shifted + CUBIC * shifted * shifted * shifted)
    return 0.5 * shifted * (1.0 + jnp.tanh(inside_arg))


def gate_slope(shifted):
    inside_arg = ROOT * (shifted + CUBIC * shifted * shifted * shifted)
    tanh_part = jnp.tanh(inside_arg)
    return 0.5 * (1.0 + tanh_part) + 0.5 * shifted * (1.0 - tanh_part * tanh_part) * ROOT * (
        1.0 + 3.0 * CUBIC * shifted * shifted
    )


def loop(first, count, step):
    if count <= 4:
        for d in range(first, count):
            step(d)
    else:
        lax.fori_loop(first, count, lambda d, c: (step(d), c)[1], 0)


def others(me, count, step):
    loop(1, count, lambda d: step(lax.rem(me + d, count)))


def signal(barrier, **where):
    pl.semaphore_signal(barrier, inc=1, device_id=where, device_id_type=MESH)


def remote(src, dst, send_sem, recv_sem, **where):
    return pltpu.make_async_remote_copy(
        src_ref=src, dst_ref=dst, send_sem=send_sem, recv_sem=recv_sem, device_id=where,
        device_id_type=MESH,
    )


ANY = pl.BlockSpec(memory_space=pl.ANY)


def nearest(l, n, d, step):
    for j in (l - d, l + d):

        @pl.when((j >= 0) & (j < n))
        def _():
            step(j)


def group_of(slots):
    return 3 if slots % 3 == 0 else 1


def slot_call(body, tables, args, in_specs, out_shape, out_spec, scratch, flops, name, grid):
    moved = sum(a.size * a.dtype.itemsize for a in args) + out_shape.size * out_shape.dtype.itemsize
    return pl.pallas_call(
        body,
        out_shape=out_shape,
        grid_spec=pltpu.PrefetchScalarGridSpec(
            num_scalar_prefetch=len(tables), grid=(grid,), in_specs=in_specs,
            out_specs=out_spec, scratch_shapes=scratch,
        ),
        compiler_params=pltpu.CompilerParams(vmem_limit_bytes=62 * 1024 * 1024),
        cost_estimate=pl.CostEstimate(flops=flops, bytes_accessed=moved, transcendentals=0),
        name=name,
    )(*tables, *args)


class Tables:
    def __init__(self, slots, layers, blocks):
        self.tgt, self.id, self.valid = 0, slots, 2 * slots
        self.prev_tgt, self.prev_id = 3 * slots, 4 * slots
        self.last_tgt = 5 * slots
        self.last_id = self.last_tgt + layers + 1
        self.size = -(-(self.last_id + blocks + 1) // 128) * 128


def slot_tables(dec_list, layers, blocks, blocks_layer):
    slots = dec_list.shape[0]
    at = Tables(slots, layers, blocks)

    def body(d_ref, o_ref):
        def clear(i, c):
            o_ref[i] = 0
            return c

        lax.fori_loop(0, at.size, clear, 0)

        def one(k, c):
            s, t, b = d_ref[k, 0], d_ref[k, 1], d_ref[k, 2]
            listed = t >= 0
            group = jnp.where(listed, t, layers)
            ident = jnp.where(listed, s * blocks_layer + b, blocks)
            o_ref[at.tgt + k] = jnp.maximum(t, 0)
            o_ref[at.id + k] = jnp.where(listed, ident, 0)
            o_ref[at.valid + k] = jnp.where(listed, 1, 0)
            o_ref[at.prev_tgt + k] = o_ref[at.last_tgt + group]
            o_ref[at.last_tgt + group] = k + 1
            o_ref[at.prev_id + k] = o_ref[at.last_id + ident]
            o_ref[at.last_id + ident] = k + 1
            return c

        lax.fori_loop(0, slots, one, 0)

    return pl.pallas_call(
        body,
        out_shape=jax.ShapeDtypeStruct((at.size,), jnp.int32),
        in_specs=[pl.BlockSpec(memory_space=pltpu.SMEM)],
        out_specs=pl.BlockSpec(memory_space=pltpu.SMEM),
        name="slot_tables",
    )(dec_list)


def chunk_count(toks):
    return next(c for c in (4, 2, 1) if toks % (16 * c) == 0 or c == 1)


def step(tables, acts_here, enc_weight, enc_bias, gate, dec_weight, targets, scale, cid):
    w_count, toks, width = acts_here.shape
    lat_dev = enc_weight.shape[1]
    slots, block, _ = dec_weight.shape
    layers = targets.shape[0]
    per_dev = lat_dev // block
    n, r_count = lax.axis_size("lay"), lax.axis_size("rep")
    assert r_count == 2
    blocks = n * per_dev
    columns = lat_dev // r_count
    half = block // r_count
    at = Tables(slots, layers, blocks)
    chunks = chunk_count(toks)
    ct = toks // chunks
    rows = w_count * ct
    wide = min(lat_dev, 512)

    cuts = next(c for c in (CUTS, 1) if width % (128 * c) == 0)
    part = width // cuts
    b_steps = layers * cuts
    b_pieces = chunks * b_steps

    split = 2 if per_dev % 2 == 0 else 1
    pb = per_dev // split
    z_steps = (n - 1) * split
    z_pieces = chunks * z_steps
    g = group_of(slots)
    groups = slots // g

    period = max(b_steps, z_steps)
    per_step = -(-slots // period)
    a_decode = A_GATE + A_SKEW * (n - 1) + A_ACROSS
    b_first = a_decode + period
    c_slots = b_first + b_steps + SKEW * (n - 1)
    c_gather = c_slots + period + C_ACROSS
    ticks = c_gather + (chunks - 1) * period + split + (n - 1) * max(split, Z_SKEW)

    def body(tab, a_ref, ew_ref, b_ref, g_ref, w_hbm, t_ref,
             po_ref, lat_hbm, lo_ref, e_hbm, eo_ref, ao_ref,
             w_ref, lat_ref, lat_now, sl_ref, p_out, p_in, e_ref, sums, own_ref, bu_in, bd_in, bu_out, bd_out,
             x_out, x_in, c_sums, made, zu_in, zd_in, zu_out, zd_out, twin_out,
             wsem, ps, pr, aus, ads, azr, axs, axr, bus, bur, bds, bdr, xs, xr, zus, zur, zds, zdr,
             ts, tr, tps, tpr, asem):
        l, w, r = lax.axis_index("lay"), lax.axis_index("wid"), lax.axis_index("rep")
        twin = 1 - r

        def weight(k):
            return pltpu.make_async_copy(w_hbm.at[k], w_ref.at[k], wsem.at[k])

        loop(0, slots, lambda k: weight(k).start())
        barrier = pltpu.get_barrier_semaphore()
        others(l, n, lambda j: signal(barrier, lay=j))
        others(w, w_count, lambda v: signal(barrier, wid=v))
        signal(barrier, rep=twin)
        sums[0] = jnp.zeros_like(sums[0])
        c_sums[0] = jnp.zeros_like(c_sums[0])
        pl.semaphore_wait(barrier, n + w_count - 1)

        def chunk(c):
            return pl.ds(pl.multiple_of(c * ct, ct), ct)

        def at_chunk(s, first, do, last=0):
            t = s - first

            @pl.when((t >= 0) & (t < chunks * period))
            def _():
                @pl.when(lax.rem(t, period) == last)
                def _():
                    do(t // period)


        def p_send(c, v):
            return remote(p_out.at[c, v], p_in.at[c, w], ps.at[c * w_count + v], pr.at[c * w_count + w], wid=v)

        def p_landed(c, v):
            return remote(p_in.at[c, v], p_in.at[c, v], ps.at[c * w_count + v], pr.at[c * w_count + v], wid=v)

        def product(c):
            held = a_ref[:, chunk(c), :].reshape(rows, width)
            for o in range(0, lat_dev, wide):
                made_here = jnp.dot(held, ew_ref[:, o:o + wide], preferred_element_type=F32).astype(BF16)
                for v in range(w_count):
                    p_out[c, v, :, o:o + wide] = made_here[v * ct:(v + 1) * ct]
            others(w, w_count, lambda v: p_send(c, v).start())

        def shard(c, j, v):
            return lat_ref.at[pl.ds(j * per_dev, per_dev), v, chunk(c)]

        def a_up(c, j):
            return remote(shard(c, j, w), shard(c, j, w), aus.at[c * n + j], azr.at[c * n + j], lay=l + 1)

        def a_dn(c, j):
            return remote(shard(c, j, w), shard(c, j, w), ads.at[c * n + j], azr.at[c * n + j], lay=l - 1)

        def across(c, j, v, source):
            return remote(shard(c, j, source), shard(c, j, source), axs.at[(c * n + j) * w_count + v],
                          axr.at[(c * n + j) * w_count + source], wid=v)

        def goes(c, j, do):
            @pl.when((j <= l) & (l < n - 1))
            def _():
                do(a_up(c, j))

            @pl.when((j >= l) & (l > 0))
            def _():
                do(a_dn(c, j))

            others(w, w_count, lambda v: do(across(c, j, v, w)))

        def gated(c):
            others(w, w_count, lambda v: p_landed(c, v).wait_recv())
            keep = g_ref[w, chunk(c), :].astype(F32)
            for b in range(per_dev):
                over = slice(b * block, (b + 1) * block)
                shifted = p_out[c, w, :, over].astype(F32) + b_ref[:, over]
                for d in range(1, w_count):
                    shifted = shifted + p_in[c, lax.rem(w + d, w_count), :, over].astype(F32)
                held = keep[:, b:b + 1]
                lat_ref[l * per_dev + b, w, chunk(c), :] = (smooth_gate(shifted) * held).astype(BF16)
                sl_ref[b, chunk(c), :] = gate_slope(shifted) * held
            goes(c, l, lambda copy: copy.start())

        def take(c, j):
            remote(shard(c, j, w), shard(c, j, w), aus.at[c * n + j], azr.at[c * n + j], lay=j).wait_recv()
            goes(c, j, lambda copy: copy.start())

        def crossed(c):
            loop(0, n, lambda j: others(w, w_count, lambda v: across(c, j, v, v).wait_recv()))
            lat_now[...] = lat_ref[:, :, chunk(c), :]


        def slot(k):
            held = lat_now[tab[at.id + k]].reshape(rows, block)
            sums[k + 1] = jnp.dot(held, w_ref[k], preferred_element_type=F32) + sums[tab[at.prev_tgt + k]]

        def emit(c):
            for t in range(layers):
                total = sums[tab[at.last_tgt + t]].astype(BF16)
                for i in range(cuts):
                    own_ref[c * b_steps + t * cuts + i] = total[:, i * part:(i + 1) * part]

        def b_up(q):
            return remote(bu_out.at[q], bu_in.at[q], bus.at[q], bur.at[q], lay=l + 1)

        def b_dn(q):
            return remote(bd_out.at[q], bd_in.at[q], bds.at[q], bdr.at[q], lay=l - 1)

        def b_inside(q):
            return (q >= 0) & (q < chunks * period) & (lax.rem(q + period * chunks, period) < b_steps)

        def b_piece(q):
            return q // period * b_steps + lax.rem(q + period * chunks, period)

        def hand_on(s):
            q, p = s - SKEW * l, s - SKEW * (n - 1 - l)
            e = s - SKEW * jnp.maximum(l, n - 1 - l)
            q_in, p_in_, e_in = b_inside(q), b_inside(p), b_inside(e)
            q, p, e = b_piece(q), b_piece(p), b_piece(e)

            @pl.when(q_in & (l > 0))
            def _():
                remote(bu_in.at[q], bu_in.at[q], bus.at[q], bur.at[q], lay=l).wait_recv()

            @pl.when(q_in & (l == 0))
            def _():
                bu_out[q] = own_ref[q]

            @pl.when(q_in & (l > 0) & (l < n - 1))
            def _():
                bu_out[q] = (own_ref[q].astype(F32) + bu_in[q].astype(F32)).astype(BF16)

            @pl.when(p_in_ & (l < n - 1))
            def _():
                remote(bd_in.at[p], bd_in.at[p], bds.at[p], bdr.at[p], lay=l).wait_recv()

            @pl.when(p_in_ & (l == n - 1))
            def _():
                bd_out[p] = own_ref[p]

            @pl.when(p_in_ & (l > 0) & (l < n - 1))
            def _():
                bd_out[p] = (own_ref[p].astype(F32) + bd_in[p].astype(F32)).astype(BF16)

            def error(total):
                c, i = e // b_steps, lax.rem(e, b_steps)
                t, i = i // cuts, lax.rem(i, cuts)
                over = pl.ds(pl.multiple_of(i * part, part), part)
                aim = t_ref[t, :, chunk(c), over].reshape(rows, part).astype(F32)
                e_ref[t, :, chunk(c), over] = ((total - aim) * scale).astype(BF16).reshape(w_count, ct, part)

            @pl.when(e_in & (l == 0))
            def _():
                error(own_ref[e].astype(F32) + bd_in[e].astype(F32))

            @pl.when(e_in & (l == n - 1))
            def _():
                error(own_ref[e].astype(F32) + bu_in[e].astype(F32))

            @pl.when(e_in & (l > 0) & (l < n - 1))
            def _():
                error(own_ref[e].astype(F32) + bu_in[e].astype(F32) + bd_in[e].astype(F32))

            @pl.when(q_in & (l < n - 1))
            def _():
                b_up(q).start()

            @pl.when(p_in_ & (l > 0))
            def _():
                b_dn(p).start()


        def x_send(c, i, v):
            where = pl.ds(i * g, g)
            return remote(x_out.at[c, v, where], x_in.at[c, w, where], xs.at[(c * groups + i) * w_count + v],
                          xr.at[(c * groups + i) * w_count + w], wid=v)

        def x_landed(c, i, v):
            where = pl.ds(i * g, g)
            return remote(x_in.at[c, v, where], x_in.at[c, v, where],
                          xs.at[(c * groups + i) * w_count + v],
                          xr.at[(c * groups + i) * w_count + v], wid=v)

        def slot_group(c, i):
            for k in [i * g + d for d in range(g)]:
                held = e_ref[tab[at.tgt + k], :, chunk(c), :].reshape(rows, width)
                back = lax.dot_general(
                    held, w_ref[k], (((1,), (1,)), ((), ())), preferred_element_type=F32
                ).astype(BF16).reshape(w_count, ct, block)
                for v in range(w_count):
                    x_out[c, v, k] = back[v]
            others(w, w_count, lambda v: x_send(c, i, v).start())

        def gather(c):
            def landed(i, carry):
                others(w, w_count, lambda v: x_landed(c, i, v).wait_recv())
                return carry

            lax.fori_loop(0, groups, landed, 0)

            def one(k, carry):
                total = c_sums[tab[at.prev_id + k]] + x_out[c, w, k].astype(F32)
                for d in range(1, w_count):
                    total = total + x_in[c, lax.rem(w + d, w_count), k].astype(F32)
                c_sums[k + 1] = total
                return carry

            lax.fori_loop(0, slots, one, 0)

            def out(b, carry):
                made[c, b] = c_sums[tab[at.last_id + b]].astype(BF16)
                return carry

            lax.fori_loop(0, blocks, out, 0)

        def z_up(q):
            return remote(zu_out.at[q], zu_in.at[q], zus.at[q], zur.at[q], lay=l + 1)

        def z_dn(q):
            return remote(zd_out.at[q], zd_in.at[q], zds.at[q], zdr.at[q], lay=l - 1)

        def z_inside(q):
            return (q >= 0) & (q < chunks * period) & (lax.rem(q + period * chunks, period) < z_steps)

        def z_piece(q):
            return q // period * z_steps + lax.rem(q + period * chunks, period)

        def own_z(q, dest):
            return made[q // z_steps, pl.ds(dest * per_dev + lax.rem(q, split) * pb, pb)].astype(F32)

        def twin_pre(c):
            return remote(twin_out.at[c], po_ref.at[r, chunk(c)], tps.at[c], tpr.at[c], rep=twin)

        def twin_landed(c):
            return remote(twin_out.at[c], po_ref.at[twin, chunk(c)], tps.at[c], tpr.at[c], rep=twin)

        def reduce_on(s):
            q, p = s - Z_SKEW * l, s - Z_SKEW * (n - 1 - l)
            q_in, p_in_ = z_inside(q), z_inside(p)
            q, p = z_piece(q), z_piece(p)
            to_up = n - 1 - lax.rem(q + z_pieces, z_steps) // split
            to_dn = lax.rem(p + z_pieces, z_steps) // split

            @pl.when(q_in & (l > 0) & (to_up >= l))
            def _():
                remote(zu_in.at[q], zu_in.at[q], zus.at[q], zur.at[q], lay=l).wait_recv()

            @pl.when(q_in & (l == 0))
            def _():
                zu_out[q] = own_z(q, to_up).astype(BF16)

            @pl.when(q_in & (l > 0) & (to_up > l))
            def _():
                zu_out[q] = (own_z(q, to_up) + zu_in[q].astype(F32)).astype(BF16)

            @pl.when(p_in_ & (l < n - 1) & (to_dn <= l))
            def _():
                remote(zd_in.at[p], zd_in.at[p], zds.at[p], zdr.at[p], lay=l).wait_recv()

            @pl.when(p_in_ & (l == n - 1))
            def _():
                zd_out[p] = own_z(p, to_dn).astype(BF16)

            @pl.when(p_in_ & (l < n - 1) & (to_dn < l))
            def _():
                zd_out[p] = (own_z(p, to_dn) + zd_in[p].astype(F32)).astype(BF16)

            off_up = (n - 1 - l) * split
            off_dn = l * split
            f = s - jnp.maximum(off_up + Z_SKEW * l, off_dn + Z_SKEW * (n - 1 - l))
            i = lax.rem(f + period * chunks, period)
            whole = (f >= 0) & (f < chunks * period) & (i < split)
            c = f // period

            def finish(total):
                blocks_here = pl.ds(i * pb, pb)
                grad = (total * sl_ref[blocks_here, chunk(c), :]).astype(BF16)
                if split == r_count:
                    @pl.when(i == r)
                    def _():
                        for b in range(pb):
                            po_ref[r, chunk(c), b * block:(b + 1) * block] = grad[b]

                    @pl.when(i != r)
                    def _():
                        for b in range(pb):
                            twin_out[c, :, b * block:(b + 1) * block] = grad[b]
                else:
                    for b in range(pb):
                        for side in range(r_count):
                            cut = grad[b][:, side * half:(side + 1) * half]

                            @pl.when(r == side)
                            def _():
                                po_ref[side, chunk(c), b * half:(b + 1) * half] = cut

                            @pl.when(r != side)
                            def _():
                                twin_out[c, :, b * half:(b + 1) * half] = cut

            def mid():
                return made[c, pl.ds(l * per_dev + i * pb, pb)].astype(F32)

            @pl.when(whole & (l == 0))
            def _():
                finish(mid() + zd_in[c * z_steps + off_dn + i].astype(F32))

            @pl.when(whole & (l == n - 1))
            def _():
                finish(mid() + zu_in[c * z_steps + off_up + i].astype(F32))

            @pl.when(whole & (l > 0) & (l < n - 1))
            def _():
                finish(mid() + zu_in[c * z_steps + off_up + i].astype(F32)
                       + zd_in[c * z_steps + off_dn + i].astype(F32))

            @pl.when(q_in & (to_up > l))
            def _():
                z_up(q).start()

            @pl.when(p_in_ & (to_dn < l))
            def _():
                z_dn(p).start()

            @pl.when(whole & (i == split - 1))
            def _():
                twin_pre(c).start()


        twins = [
            remote(lat_ref.at[:, :, :, pl.ds(pl.multiple_of(twin * half, half), half)], lo_ref,
                   ts.at[0], tr.at[0], rep=twin),
            remote(e_ref, eo_ref, ts.at[1], tr.at[1], rep=twin),
        ] + [
            remote(a_ref.at[v], ao_ref.at[lax.rem(v - w + w_count, w_count), r], ts.at[2 + v], tr.at[2 + v],
                   rep=twin)
            for v in range(w_count)
        ]
        mine = [
            pltpu.make_async_copy(lat_ref, lat_hbm, asem.at[0]),
            pltpu.make_async_copy(e_ref, e_hbm, asem.at[1]),
        ] + [
            pltpu.make_async_copy(
                a_ref.at[v], ao_ref.at[lax.rem(v - w + w_count, w_count), r], asem.at[2 + v])
            for v in range(w_count)
        ]

        def tick(s, carry):
            def arrive(d):
                at_chunk(s, A_GATE + A_SKEW * d, lambda c: nearest(l, n, d, lambda j: take(c, j)))

            loop(1, n, arrive)
            hand_on(s - b_first)
            at_chunk(s, c_gather, gather)
            reduce_on(s - c_gather)
            at_chunk(s, A_GATE, gated)
            at_chunk(s, 0, product)

            t = s - c_slots

            @pl.when((t >= 0) & (t < chunks * period))
            def _():
                c, i = t // period, lax.rem(t, period)
                lax.fori_loop(
                    (i * groups + period - 1) // period, ((i + 1) * groups + period - 1) // period,
                    lambda j, z: (slot_group(c, j), z)[1], 0,
                )

            u = s - a_decode

            @pl.when((u >= 0) & (u < chunks * period))
            def _():
                c, i = u // period, lax.rem(u, period)

                @pl.when(i == 0)
                def _():
                    crossed(c)

                for d in range(per_step):
                    @pl.when(i * per_step + d < slots)
                    def _():
                        slot(i * per_step + d)

                @pl.when(i == period - 1)
                def _():
                    emit(c)

            @pl.when(s == a_decode - 1)
            def _():
                loop(0, slots, lambda k: weight(k).wait())
                for v in range(w_count):
                    twins[2 + v].start()
                    mine[2 + v].start()

            @pl.when(s == a_decode + (chunks - 1) * period)
            def _():
                twins[0].start()
                mine[0].start()

            @pl.when(s == c_slots + (chunks - 1) * period)
            def _():
                twins[1].start()
                mine[1].start()

            return carry

        lax.fori_loop(0, ticks, tick, 0)

        def a_sent(q, carry):
            goes(q // n, lax.rem(q, n), lambda copy: copy.wait_send())
            return carry

        lax.fori_loop(0, chunks * n, a_sent, 0)

        def b_sent(q, carry):
            @pl.when(l < n - 1)
            def _():
                b_up(q).wait_send()

            @pl.when(l > 0)
            def _():
                b_dn(q).wait_send()

            return carry

        lax.fori_loop(0, b_pieces, b_sent, 0)

        def z_sent(q, carry):
            to_up = n - 1 - lax.rem(q, z_steps) // split
            to_dn = lax.rem(q, z_steps) // split

            @pl.when(to_up > l)
            def _():
                z_up(q).wait_send()

            @pl.when(to_dn < l)
            def _():
                z_dn(q).wait_send()

            return carry

        lax.fori_loop(0, z_pieces, z_sent, 0)

        def x_sent(q, carry):
            others(w, w_count, lambda v: x_send(q // groups, lax.rem(q, groups), v).wait_send())
            return carry

        lax.fori_loop(0, chunks * groups, x_sent, 0)
        for c in range(chunks):
            others(w, w_count, lambda v: p_send(c, v).wait_send())
            twin_landed(c).wait()
        for copy in twins + mine:
            copy.wait()

    b_piece_shape = (b_pieces, rows, part)
    z_piece_shape = (z_pieces, pb, ct, block)
    x_shape = (chunks, w_count, slots, ct, block)
    lat_shape = (blocks, w_count, toks, block)
    vmem = pl.BlockSpec(memory_space=pltpu.VMEM)
    dma = pltpu.SemaphoreType.DMA
    x_sems = chunks * groups * w_count
    return pl.pallas_call(
        body,
        out_shape=(
            jax.ShapeDtypeStruct((r_count, toks, columns), BF16),
            jax.ShapeDtypeStruct(lat_shape, BF16),
            jax.ShapeDtypeStruct(lat_shape[:3] + (half,), BF16),
            jax.ShapeDtypeStruct(targets.shape, BF16),
            jax.ShapeDtypeStruct(targets.shape, BF16),
            jax.ShapeDtypeStruct((w_count, r_count, toks, width), acts_here.dtype),
        ),
        in_specs=[pl.BlockSpec(memory_space=pltpu.SMEM), vmem, vmem, vmem, vmem, ANY, vmem],
        out_specs=(vmem, ANY, ANY, ANY, ANY, ANY),
        scratch_shapes=[
            pltpu.VMEM(dec_weight.shape, BF16),
            pltpu.VMEM(lat_shape, BF16),
            pltpu.VMEM((blocks, w_count, ct, block), BF16),
            pltpu.VMEM((per_dev, toks, block), F32),
            pltpu.VMEM((chunks, w_count, ct, lat_dev), BF16),
            pltpu.VMEM((chunks, w_count, ct, lat_dev), BF16),
            pltpu.VMEM(targets.shape, BF16),
            pltpu.VMEM((slots + 1, rows, width), F32),
        ] + [pltpu.VMEM(b_piece_shape, BF16)] * 5 + [
            pltpu.VMEM(x_shape, BF16),
            pltpu.VMEM(x_shape, BF16),
            pltpu.VMEM((slots + 1, ct, block), F32),
            pltpu.VMEM((chunks, blocks, ct, block), BF16),
        ] + [pltpu.VMEM(z_piece_shape, BF16)] * 4 + [
            pltpu.VMEM((chunks, ct, columns), BF16),
            dma((slots,)), dma((chunks * w_count,)), dma((chunks * w_count,)),
        ] + [dma((chunks * n,))] * 3 + [dma((chunks * n * w_count,))] * 2 + [dma((b_pieces,))] * 4
        + [dma((x_sems,))] * 2 + [dma((z_pieces,))] * 4 + [
            dma((2 + w_count,)), dma((2 + w_count,)), dma((chunks,)), dma((chunks,)), dma((2 + w_count,)),
        ],
        compiler_params=pltpu.CompilerParams(
            collective_id=cid, has_side_effects=True, vmem_limit_bytes=67043328
        ),
        name="step",
    )(tables, acts_here, enc_weight, enc_bias, gate, dec_weight, targets)


def decoder_grads(ids, tgt, valid, rep, lat, lat_twin, err, err_twin, slots):
    layers, toks, width = err.shape
    blocks, _, half = lat_twin.shape
    g = group_of(slots)

    def body(i_ref, t_ref, v_ref, r_ref, l_ref, lt_ref, e_ref, et_ref, o_ref):
        over = (((0,), (0,)), ((), ()))
        for i in range(g):
            k = pl.program_id(0) * g + i

            @pl.when(v_ref[k] > 0)
            def _():
                t, b = t_ref[k], i_ref[k]
                o_ref[i] = lax.dot_general(
                    l_ref[b], e_ref[t], over, preferred_element_type=F32
                ) + lax.dot_general(lt_ref[b], et_ref[t], over, preferred_element_type=F32)

            @pl.when(v_ref[k] == 0)
            def _():
                o_ref[i] = jnp.zeros_like(o_ref[i])

    return slot_call(
        body, (ids, tgt, valid, rep), (lat, lat_twin, err, err_twin),
        [pl.BlockSpec((blocks, toks, half), lambda k, i, t, v, r: (0, 0, r[0])),
         pl.BlockSpec((blocks, toks, half), lambda k, i, t, v, r: (0, 0, 0)),
         pl.BlockSpec((layers, toks, width), lambda k, i, t, v, r: (0, 0, 0)),
         pl.BlockSpec((layers, toks, width), lambda k, i, t, v, r: (0, 0, 0))],
        jax.ShapeDtypeStruct((slots, half, width), F32),
        pl.BlockSpec((g, half, width), lambda k, i, t, v, r: (k, 0, 0)),
        [], 4 * slots * toks * half * width, "decoder_grads", slots // g,
    )


def local(acts, targets, enc_weight, enc_bias, gate_mask, dec_list, dec_weight):
    layers, tok_rows, width_part = acts.shape
    lat_dev = enc_weight.shape[1]
    slots, block, _ = dec_weight.shape
    per_dev = lat_dev // block
    n, w_count, r_count = lax.axis_size("lay"), lax.axis_size("wid"), lax.axis_size("rep")
    lay, wid, rep = lax.axis_index("lay"), lax.axis_index("wid"), lax.axis_index("rep")
    lat_total = lat_dev * n
    blocks_total = lat_total // block
    latents_layer = lat_total // layers
    blocks_layer = latents_layer // block
    toks = tok_rows // w_count

    tgt = dec_list[:, 1]
    valid = (tgt >= 0).astype(jnp.int32)
    ids = jnp.maximum(dec_list[:, 0] * blocks_layer + dec_list[:, 2], 0)
    tgt = jnp.maximum(tgt, 0)

    here = lax.dynamic_index_in_dim(acts, lay * lat_dev // latents_layer, 0, keepdims=False)
    here = here.reshape(w_count, toks, width_part)
    scale = float(tok_rows * r_count) ** (-0.5)
    pre_mine, lat, lat_twin, err, err_twin, acts_all = step(
        slot_tables(dec_list, layers, blocks_total, blocks_layer), here, enc_weight,
        enc_bias.reshape(1, lat_dev), gate_mask.reshape(w_count, toks, per_dev), dec_weight,
        targets.reshape(layers, w_count, toks, width_part), scale, 0,
    )
    pre_all = [pre_mine] + [
        lax.ppermute(pre_mine, "wid", [(i, (i - d) % w_count) for i in range(w_count)])
        for d in range(1, w_count)
    ]
    half = block // r_count
    dec_out = decoder_grads(
        ids, tgt, valid, rep.reshape(1).astype(jnp.int32),
        lat.reshape(blocks_total, tok_rows, block), lat_twin.reshape(blocks_total, tok_rows, half),
        err.reshape(layers, tok_rows, width_part), err_twin.reshape(layers, tok_rows, width_part), slots,
    )
    columns = lat_dev // r_count
    pre_all = jnp.stack(pre_all).reshape(r_count * tok_rows, columns)
    enc_out = lax.dot_general(
        acts_all.reshape(r_count * tok_rows, width_part), pre_all, (((0,), (0,)), ((), ())),
        preferred_element_type=F32,
    )
    bias_out = jnp.sum(pre_all.astype(F32), axis=0)
    return (enc_out, bias_out, dec_out)


def solution(mesh):
    return jax.shard_map(
        local,
        mesh=mesh,
        in_specs=(
            P(None, ("grp", "rep"), "wid"),
            P(None, ("grp", "rep"), "wid"),
            P("wid", "lay"),
            P("lay"),
            P(("grp", "rep"), "lay"),
            P("lay", None),
            P("lay", None, "wid"),
        ),
        out_specs=(
            P(("grp", "wid"), ("lay", "rep")),
            P(("grp", "lay", "rep")),
            P(("grp", "lay"), "rep", "wid"),
        ),
        check_vma=False,
    )
```

```python
import jax
import jax.numpy as jnp
from jax import lax
from jax.experimental import pallas as pl
from jax.experimental.pallas import tpu as pltpu
from jax.sharding import PartitionSpec as P

ROOT = 0.7978845608028654
CUBIC = 0.044715
MESH = pl.DeviceIdType.MESH
BF16 = jnp.bfloat16
F32 = jnp.float32
CUTS = 2
SKEW = 4
Z_SKEW = 5
PERIOD = 8
A_GATE = 14
A_SKEW = 3
A_ACROSS = 7
C_ACROSS = 3


def smooth_gate(shifted):
    inside_arg = ROOT * (shifted + CUBIC * shifted * shifted * shifted)
    return 0.5 * shifted * (1.0 + jnp.tanh(inside_arg))


def gate_slope(shifted):
    inside_arg = ROOT * (shifted + CUBIC * shifted * shifted * shifted)
    tanh_part = jnp.tanh(inside_arg)
    return 0.5 * (1.0 + tanh_part) + 0.5 * shifted * (1.0 - tanh_part * tanh_part) * ROOT * (
        1.0 + 3.0 * CUBIC * shifted * shifted
    )


def loop(first, count, step):
    if count <= 4:
        for d in range(first, count):
            step(d)
    else:
        lax.fori_loop(first, count, lambda d, c: (step(d), c)[1], 0)


def others(me, count, step):
    loop(1, count, lambda d: step(lax.rem(me + d, count)))


def signal(barrier, **where):
    pl.semaphore_signal(barrier, inc=1, device_id=where, device_id_type=MESH)


def remote(src, dst, send_sem, recv_sem, **where):
    return pltpu.make_async_remote_copy(
        src_ref=src, dst_ref=dst, send_sem=send_sem, recv_sem=recv_sem, device_id=where,
        device_id_type=MESH,
    )


ANY = pl.BlockSpec(memory_space=pl.ANY)


def nearest(l, n, d, step):
    for j in (l - d, l + d):

        @pl.when((j >= 0) & (j < n))
        def _():
            step(j)


def group_of(slots):
    return 3 if slots % 3 == 0 else 1


def slot_call(body, tables, args, in_specs, out_shape, out_spec, scratch, flops, name, grid):
    moved = sum(a.size * a.dtype.itemsize for a in args) + out_shape.size * out_shape.dtype.itemsize
    return pl.pallas_call(
        body,
        out_shape=out_shape,
        grid_spec=pltpu.PrefetchScalarGridSpec(
            num_scalar_prefetch=len(tables), grid=(grid,), in_specs=in_specs,
            out_specs=out_spec, scratch_shapes=scratch,
        ),
        compiler_params=pltpu.CompilerParams(vmem_limit_bytes=62 * 1024 * 1024),
        cost_estimate=pl.CostEstimate(flops=flops, bytes_accessed=moved, transcendentals=0),
        name=name,
    )(*tables, *args)


class Tables:
    def __init__(self, slots, layers, blocks):
        self.tgt, self.id, self.raw = 0, slots, 2 * slots
        self.prev_tgt, self.prev_id = 3 * slots, 4 * slots
        self.last_tgt = 5 * slots
        self.last_id = self.last_tgt + layers
        self.size = -(-(self.last_id + blocks) // 128) * 128


def chunk_count(toks):
    return next(c for c in (4, 2, 1) if toks % (16 * c) == 0 or c == 1)


def step(acts, enc_weight, enc_bias, gate, dec_list, dec_weight, targets, scale, cid):
    layers, w_count, toks, width = acts.shape
    lat_dev = enc_weight.shape[1]
    slots, block, _ = dec_weight.shape
    per_dev = lat_dev // block
    n, r_count = lax.axis_size("lay"), lax.axis_size("rep")
    assert r_count == 2
    blocks = n * per_dev
    blocks_layer = blocks // layers
    columns = lat_dev // r_count
    half = block // r_count
    at = Tables(slots, layers, blocks)
    chunks = chunk_count(toks)
    ct = toks // chunks
    rows = w_count * ct
    wide = min(lat_dev, 512)

    cuts = next(c for c in (CUTS, 1) if width % (128 * c) == 0)
    part = width // cuts
    b_steps = layers * cuts
    b_pieces = chunks * b_steps

    split = 2 if per_dev % 2 == 0 else 1
    pb = per_dev // split
    z_steps = (n - 1) * split
    z_pieces = chunks * z_steps
    g = group_of(slots)
    groups = slots // g

    period = max(b_steps, z_steps, PERIOD)
    per_step = -(-slots // period)
    a_decode = A_GATE + A_SKEW * (n - 1) + A_ACROSS
    b_first = a_decode + period
    c_slots = b_first + b_steps + SKEW * (n - 1)
    c_gather = c_slots + period + C_ACROSS
    ticks = c_gather + (chunks - 1) * period + split + (n - 1) * max(split, Z_SKEW)

    table_slots = -(-slots // (a_decode - 1))
    table_blocks = -(-blocks // (a_decode - 1))

    def body(d_ref, a_hbm, ew_hbm, b_ref, g_ref, w_hbm, t_ref,
             tab, po_ref, lo_ref, eo_ref, ao_ref,
             a_ref, ew_ref, keep_ref, w_ref, lat_ref, lat_now, sl_ref, p_out, p_in, e_ref, sums, own_ref, bu_in, bd_in, bu_out, bd_out,
             x_out, x_in, c_sums, made, zu_in, zd_in, zu_out, zd_out, twin_out,
             wsem, ps, pr, aus, ads, azr, axs, axr, bus, bur, bds, bdr, xs, xr, zus, zur, zds, zdr,
             ts, tr, tps, tpr, asem, isem):
        l, w, r = lax.axis_index("lay"), lax.axis_index("wid"), lax.axis_index("rep")
        twin = 1 - r

        def weight(k):
            return pltpu.make_async_copy(w_hbm.at[k], w_ref.at[k], wsem.at[k])

        layer = l * per_dev // blocks_layer
        acts_in = pltpu.make_async_copy(a_hbm.at[layer], a_ref, isem.at[0])
        enc_in = [
            pltpu.make_async_copy(ew_hbm.at[:, o:o + wide], ew_ref.at[:, o:o + wide], isem.at[1 + i])
            for i, o in enumerate(range(0, lat_dev, wide))
        ]
        acts_in.start()
        for copy in enc_in:
            copy.start()
        loop(0, slots, lambda k: weight(k).start())
        barrier = pltpu.get_barrier_semaphore()
        others(l, n, lambda j: signal(barrier, lay=j))
        others(w, w_count, lambda v: signal(barrier, wid=v))
        signal(barrier, rep=twin)
        sums[0] = jnp.zeros_like(sums[0])
        c_sums[0] = jnp.zeros_like(c_sums[0])
        keep_ref[...] = g_ref[...].astype(F32).T

        def listed(k, carry):
            t = d_ref[1, k]
            raw = jnp.where(t >= 0, d_ref[0, k] * blocks_layer + d_ref[2, k], -1)
            tab[at.tgt + k] = jnp.maximum(t, 0)
            tab[at.raw + k] = raw
            tab[at.id + k] = jnp.maximum(raw, 0)
            return carry

        lax.fori_loop(0, slots, listed, 0)

        def last_of(which, value, below):
            found = jnp.int32(0)
            for j in range(slots):
                found = jnp.where((which(j) == value) & (j < below), j + 1, found)
            return found

        def target(j):
            return d_ref[1, j]

        def named(j):
            return tab[at.raw + j]

        for t in range(layers):
            tab[at.last_tgt + t] = last_of(target, t, slots)

        def some_tables(s):
            for d in range(table_slots):
                k = s * table_slots + d

                @pl.when(k < slots)
                def _():
                    tab[at.prev_tgt + k] = last_of(target, target(k), k)
                    tab[at.prev_id + k] = last_of(named, named(k), k)

            for d in range(table_blocks):
                b = s * table_blocks + d

                @pl.when(b < blocks)
                def _():
                    tab[at.last_id + b] = last_of(named, b, slots)

        pl.semaphore_wait(barrier, n + w_count - 1)
        acts_in.wait()

        def chunk(c):
            return pl.ds(pl.multiple_of(c * ct, ct), ct)

        def at_chunk(s, first, do, last=0):
            t = s - first

            @pl.when((t >= 0) & (t < chunks * period))
            def _():
                @pl.when(lax.rem(t, period) == last)
                def _():
                    do(t // period)


        def p_send(c, v):
            return remote(p_out.at[c, v], p_in.at[c, w], ps.at[c * w_count + v], pr.at[c * w_count + w], wid=v)

        def p_landed(c, v):
            return remote(p_in.at[c, v], p_in.at[c, v], ps.at[c * w_count + v], pr.at[c * w_count + v], wid=v)

        def product(c):
            held = a_ref[:, chunk(c), :].reshape(rows, width)
            for i, o in enumerate(range(0, lat_dev, wide)):
                @pl.when(c == 0)
                def _():
                    enc_in[i].wait()

                made_here = jnp.dot(held, ew_ref[:, o:o + wide], preferred_element_type=F32).astype(BF16)
                for v in range(w_count):
                    p_out[c, v, :, o:o + wide] = made_here[v * ct:(v + 1) * ct]
            others(w, w_count, lambda v: p_send(c, v).start())

        def shard(c, j, v):
            return lat_ref.at[pl.ds(j * per_dev, per_dev), v, chunk(c)]

        def a_up(c, j):
            return remote(shard(c, j, w), shard(c, j, w), aus.at[c * n + j], azr.at[c * n + j], lay=l + 1)

        def a_dn(c, j):
            return remote(shard(c, j, w), shard(c, j, w), ads.at[c * n + j], azr.at[c * n + j], lay=l - 1)

        def across(c, j, v, source):
            return remote(shard(c, j, source), shard(c, j, source), axs.at[(c * n + j) * w_count + v],
                          axr.at[(c * n + j) * w_count + source], wid=v)

        def goes(c, j, do):
            @pl.when((j <= l) & (l < n - 1))
            def _():
                do(a_up(c, j))

            @pl.when((j >= l) & (l > 0))
            def _():
                do(a_dn(c, j))

            others(w, w_count, lambda v: do(across(c, j, v, w)))

        def gated(c):
            others(w, w_count, lambda v: p_landed(c, v).wait_recv())
            keep = keep_ref[pl.ds(pl.multiple_of(w * toks + c * ct, ct), ct), :]
            for b in range(per_dev):
                over = slice(b * block, (b + 1) * block)
                shifted = p_out[c, w, :, over].astype(F32) + b_ref[:, over]
                for d in range(1, w_count):
                    shifted = shifted + p_in[c, lax.rem(w + d, w_count), :, over].astype(F32)
                held = keep[:, b:b + 1]
                lat_ref[l * per_dev + b, w, chunk(c), :] = (smooth_gate(shifted) * held).astype(BF16)
                sl_ref[b, chunk(c), :] = gate_slope(shifted) * held
            goes(c, l, lambda copy: copy.start())

        def take(c, j):
            remote(shard(c, j, w), shard(c, j, w), aus.at[c * n + j], azr.at[c * n + j], lay=j).wait_recv()
            goes(c, j, lambda copy: copy.start())

        def crossed(c):
            loop(0, n, lambda j: others(w, w_count, lambda v: across(c, j, v, v).wait_recv()))
            lat_now[...] = lat_ref[:, :, chunk(c), :]


        def slot(k):
            held = lat_now[tab[at.id + k]].reshape(rows, block)
            sums[k + 1] = jnp.dot(held, w_ref[k], preferred_element_type=F32) + sums[tab[at.prev_tgt + k]]

        def emit(c):
            for t in range(layers):
                total = sums[tab[at.last_tgt + t]].astype(BF16)
                for i in range(cuts):
                    own_ref[c * b_steps + t * cuts + i] = total[:, i * part:(i + 1) * part]

        def b_up(q):
            return remote(bu_out.at[q], bu_in.at[q], bus.at[q], bur.at[q], lay=l + 1)

        def b_dn(q):
            return remote(bd_out.at[q], bd_in.at[q], bds.at[q], bdr.at[q], lay=l - 1)

        def b_inside(q):
            return (q >= 0) & (q < chunks * period) & (lax.rem(q + period * chunks, period) < b_steps)

        def b_piece(q):
            return q // period * b_steps + lax.rem(q + period * chunks, period)

        def hand_on(s):
            q, p = s - SKEW * l, s - SKEW * (n - 1 - l)
            e = s - SKEW * jnp.maximum(l, n - 1 - l)
            q_in, p_in_, e_in = b_inside(q), b_inside(p), b_inside(e)
            q, p, e = b_piece(q), b_piece(p), b_piece(e)

            @pl.when(q_in & (l > 0))
            def _():
                remote(bu_in.at[q], bu_in.at[q], bus.at[q], bur.at[q], lay=l).wait_recv()

            @pl.when(q_in & (l == 0))
            def _():
                bu_out[q] = own_ref[q]

            @pl.when(q_in & (l > 0) & (l < n - 1))
            def _():
                bu_out[q] = (own_ref[q].astype(F32) + bu_in[q].astype(F32)).astype(BF16)

            @pl.when(p_in_ & (l < n - 1))
            def _():
                remote(bd_in.at[p], bd_in.at[p], bds.at[p], bdr.at[p], lay=l).wait_recv()

            @pl.when(p_in_ & (l == n - 1))
            def _():
                bd_out[p] = own_ref[p]

            @pl.when(p_in_ & (l > 0) & (l < n - 1))
            def _():
                bd_out[p] = (own_ref[p].astype(F32) + bd_in[p].astype(F32)).astype(BF16)

            def error(total):
                c, i = e // b_steps, lax.rem(e, b_steps)
                t, i = i // cuts, lax.rem(i, cuts)
                over = pl.ds(pl.multiple_of(i * part, part), part)
                aim = t_ref[t, :, chunk(c), over].reshape(rows, part).astype(F32)
                e_ref[t, :, chunk(c), over] = ((total - aim) * scale).astype(BF16).reshape(w_count, ct, part)

            @pl.when(e_in & (l == 0))
            def _():
                error(own_ref[e].astype(F32) + bd_in[e].astype(F32))

            @pl.when(e_in & (l == n - 1))
            def _():
                error(own_ref[e].astype(F32) + bu_in[e].astype(F32))

            @pl.when(e_in & (l > 0) & (l < n - 1))
            def _():
                error(own_ref[e].astype(F32) + bu_in[e].astype(F32) + bd_in[e].astype(F32))

            @pl.when(q_in & (l < n - 1))
            def _():
                b_up(q).start()

            @pl.when(p_in_ & (l > 0))
            def _():
                b_dn(p).start()


        def x_send(c, i, v):
            where = pl.ds(i * g, g)
            return remote(x_out.at[c, v, where], x_in.at[c, w, where], xs.at[(c * groups + i) * w_count + v],
                          xr.at[(c * groups + i) * w_count + w], wid=v)

        def x_landed(c, i, v):
            where = pl.ds(i * g, g)
            return remote(x_in.at[c, v, where], x_in.at[c, v, where],
                          xs.at[(c * groups + i) * w_count + v],
                          xr.at[(c * groups + i) * w_count + v], wid=v)

        def slot_group(c, i):
            for k in [i * g + d for d in range(g)]:
                held = e_ref[tab[at.tgt + k], :, chunk(c), :].reshape(rows, width)
                back = lax.dot_general(
                    held, w_ref[k], (((1,), (1,)), ((), ())), preferred_element_type=F32
                ).astype(BF16).reshape(w_count, ct, block)
                for v in range(w_count):
                    x_out[c, v, k] = back[v]
            others(w, w_count, lambda v: x_send(c, i, v).start())

        def gather(c):
            def landed(i, carry):
                others(w, w_count, lambda v: x_landed(c, i, v).wait_recv())
                return carry

            lax.fori_loop(0, groups, landed, 0)

            def one(k, carry):
                total = c_sums[tab[at.prev_id + k]] + x_out[c, w, k].astype(F32)
                for d in range(1, w_count):
                    total = total + x_in[c, lax.rem(w + d, w_count), k].astype(F32)
                c_sums[k + 1] = total
                return carry

            lax.fori_loop(0, slots, one, 0)

            def out(b, carry):
                made[c, b] = c_sums[tab[at.last_id + b]].astype(BF16)
                return carry

            lax.fori_loop(0, blocks, out, 0)

        def z_up(q):
            return remote(zu_out.at[q], zu_in.at[q], zus.at[q], zur.at[q], lay=l + 1)

        def z_dn(q):
            return remote(zd_out.at[q], zd_in.at[q], zds.at[q], zdr.at[q], lay=l - 1)

        def z_inside(q):
            return (q >= 0) & (q < chunks * period) & (lax.rem(q + period * chunks, period) < z_steps)

        def z_piece(q):
            return q // period * z_steps + lax.rem(q + period * chunks, period)

        def own_z(q, dest):
            return made[q // z_steps, pl.ds(dest * per_dev + lax.rem(q, split) * pb, pb)].astype(F32)

        def twin_pre(c):
            return remote(twin_out.at[c], po_ref.at[r, chunk(c)], tps.at[c], tpr.at[c], rep=twin)

        def twin_landed(c):
            return remote(twin_out.at[c], po_ref.at[twin, chunk(c)], tps.at[c], tpr.at[c], rep=twin)

        def reduce_on(s):
            q, p = s - Z_SKEW * l, s - Z_SKEW * (n - 1 - l)
            q_in, p_in_ = z_inside(q), z_inside(p)
            q, p = z_piece(q), z_piece(p)
            to_up = n - 1 - lax.rem(q + z_pieces, z_steps) // split
            to_dn = lax.rem(p + z_pieces, z_steps) // split

            @pl.when(q_in & (l > 0) & (to_up >= l))
            def _():
                remote(zu_in.at[q], zu_in.at[q], zus.at[q], zur.at[q], lay=l).wait_recv()

            @pl.when(q_in & (l == 0))
            def _():
                zu_out[q] = own_z(q, to_up).astype(BF16)

            @pl.when(q_in & (l > 0) & (to_up > l))
            def _():
                zu_out[q] = (own_z(q, to_up) + zu_in[q].astype(F32)).astype(BF16)

            @pl.when(p_in_ & (l < n - 1) & (to_dn <= l))
            def _():
                remote(zd_in.at[p], zd_in.at[p], zds.at[p], zdr.at[p], lay=l).wait_recv()

            @pl.when(p_in_ & (l == n - 1))
            def _():
                zd_out[p] = own_z(p, to_dn).astype(BF16)

            @pl.when(p_in_ & (l < n - 1) & (to_dn < l))
            def _():
                zd_out[p] = (own_z(p, to_dn) + zd_in[p].astype(F32)).astype(BF16)

            off_up = (n - 1 - l) * split
            off_dn = l * split
            f = s - jnp.maximum(off_up + Z_SKEW * l, off_dn + Z_SKEW * (n - 1 - l))
            i = lax.rem(f + period * chunks, period)
            whole = (f >= 0) & (f < chunks * period) & (i < split)
            c = f // period

            def finish(total):
                blocks_here = pl.ds(i * pb, pb)
                grad = (total * sl_ref[blocks_here, chunk(c), :]).astype(BF16)
                if split == r_count:
                    @pl.when(i == r)
                    def _():
                        for b in range(pb):
                            po_ref[r, chunk(c), b * block:(b + 1) * block] = grad[b]

                    @pl.when(i != r)
                    def _():
                        for b in range(pb):
                            twin_out[c, :, b * block:(b + 1) * block] = grad[b]
                else:
                    for b in range(pb):
                        for side in range(r_count):
                            cut = grad[b][:, side * half:(side + 1) * half]

                            @pl.when(r == side)
                            def _():
                                po_ref[side, chunk(c), b * half:(b + 1) * half] = cut

                            @pl.when(r != side)
                            def _():
                                twin_out[c, :, b * half:(b + 1) * half] = cut

            def mid():
                return made[c, pl.ds(l * per_dev + i * pb, pb)].astype(F32)

            @pl.when(whole & (l == 0))
            def _():
                finish(mid() + zd_in[c * z_steps + off_dn + i].astype(F32))

            @pl.when(whole & (l == n - 1))
            def _():
                finish(mid() + zu_in[c * z_steps + off_up + i].astype(F32))

            @pl.when(whole & (l > 0) & (l < n - 1))
            def _():
                finish(mid() + zu_in[c * z_steps + off_up + i].astype(F32)
                       + zd_in[c * z_steps + off_dn + i].astype(F32))

            @pl.when(q_in & (to_up > l))
            def _():
                z_up(q).start()

            @pl.when(p_in_ & (to_dn < l))
            def _():
                z_dn(p).start()

            @pl.when(whole & (i == split - 1))
            def _():
                twin_pre(c).start()


        twins = [
            remote(lat_ref.at[:, :, :, pl.ds(pl.multiple_of(twin * half, half), half)], lo_ref.at[:, r],
                   ts.at[0], tr.at[0], rep=twin),
            remote(e_ref, eo_ref.at[:, r], ts.at[1], tr.at[1], rep=twin),
        ] + [
            remote(a_ref.at[v], ao_ref.at[lax.rem(v - w + w_count, w_count), r], ts.at[2 + v], tr.at[2 + v],
                   rep=twin)
            for v in range(w_count)
        ]
        mine = [
            pltpu.make_async_copy(
                lat_ref.at[:, :, :, pl.ds(pl.multiple_of(r * half, half), half)], lo_ref.at[:, r], asem.at[0]),
            pltpu.make_async_copy(e_ref, eo_ref.at[:, r], asem.at[1]),
        ] + [
            pltpu.make_async_copy(
                a_ref.at[v], ao_ref.at[lax.rem(v - w + w_count, w_count), r], asem.at[2 + v])
            for v in range(w_count)
        ]

        def tick(s, carry):
            def arrive(d):
                at_chunk(s, A_GATE + A_SKEW * d, lambda c: nearest(l, n, d, lambda j: take(c, j)))

            loop(1, n, arrive)
            hand_on(s - b_first)
            at_chunk(s, c_gather, gather)
            reduce_on(s - c_gather)
            at_chunk(s, A_GATE, gated)
            at_chunk(s, 0, product)

            @pl.when(s < a_decode - 1)
            def _():
                some_tables(s)

            t = s - c_slots

            @pl.when((t >= 0) & (t < chunks * period))
            def _():
                c, i = t // period, lax.rem(t, period)
                lax.fori_loop(
                    (i * groups + period - 1) // period, ((i + 1) * groups + period - 1) // period,
                    lambda j, z: (slot_group(c, j), z)[1], 0,
                )

            u = s - a_decode

            @pl.when((u >= 0) & (u < chunks * period))
            def _():
                c, i = u // period, lax.rem(u, period)

                @pl.when(i == 0)
                def _():
                    crossed(c)

                for d in range(per_step):
                    @pl.when(i * per_step + d < slots)
                    def _():
                        slot(i * per_step + d)

                @pl.when(i == period - 1)
                def _():
                    emit(c)

            @pl.when(s == a_decode - 1)
            def _():
                loop(0, slots, lambda k: weight(k).wait())
                for v in range(w_count):
                    twins[2 + v].start()
                    mine[2 + v].start()

            @pl.when(s == a_decode + (chunks - 1) * period)
            def _():
                twins[0].start()
                mine[0].start()

            @pl.when(s == c_slots + (chunks - 1) * period)
            def _():
                twins[1].start()
                mine[1].start()

            return carry

        lax.fori_loop(0, ticks, tick, 0)

        def a_sent(q, carry):
            goes(q // n, lax.rem(q, n), lambda copy: copy.wait_send())
            return carry

        lax.fori_loop(0, chunks * n, a_sent, 0)

        def b_sent(q, carry):
            @pl.when(l < n - 1)
            def _():
                b_up(q).wait_send()

            @pl.when(l > 0)
            def _():
                b_dn(q).wait_send()

            return carry

        lax.fori_loop(0, b_pieces, b_sent, 0)

        def z_sent(q, carry):
            to_up = n - 1 - lax.rem(q, z_steps) // split
            to_dn = lax.rem(q, z_steps) // split

            @pl.when(to_up > l)
            def _():
                z_up(q).wait_send()

            @pl.when(to_dn < l)
            def _():
                z_dn(q).wait_send()

            return carry

        lax.fori_loop(0, z_pieces, z_sent, 0)

        def x_sent(q, carry):
            others(w, w_count, lambda v: x_send(q // groups, lax.rem(q, groups), v).wait_send())
            return carry

        lax.fori_loop(0, chunks * groups, x_sent, 0)
        for c in range(chunks):
            others(w, w_count, lambda v: p_send(c, v).wait_send())
            twin_landed(c).wait()
        for copy in twins + mine:
            copy.wait()

    b_piece_shape = (b_pieces, rows, part)
    z_piece_shape = (z_pieces, pb, ct, block)
    x_shape = (chunks, w_count, slots, ct, block)
    lat_shape = (blocks, w_count, toks, block)
    vmem = pl.BlockSpec(memory_space=pltpu.VMEM)
    smem = pl.BlockSpec(memory_space=pltpu.SMEM)
    dma = pltpu.SemaphoreType.DMA
    x_sems = chunks * groups * w_count
    return pl.pallas_call(
        body,
        out_shape=(
            jax.ShapeDtypeStruct((at.size,), jnp.int32),
            jax.ShapeDtypeStruct((r_count, toks, columns), BF16),
            jax.ShapeDtypeStruct((blocks, r_count, w_count, toks, half), BF16),
            jax.ShapeDtypeStruct((layers, r_count, w_count, toks, width), BF16),
            jax.ShapeDtypeStruct((w_count, r_count, toks, width), BF16),
        ),
        in_specs=[smem, ANY, ANY, vmem, vmem, ANY, vmem],
        out_specs=(smem, vmem, ANY, ANY, ANY),
        scratch_shapes=[
            pltpu.VMEM((w_count, toks, width), BF16),
            pltpu.VMEM(enc_weight.shape, BF16),
            pltpu.VMEM((w_count * toks, per_dev), F32),
            pltpu.VMEM(dec_weight.shape, BF16),
            pltpu.VMEM(lat_shape, BF16),
            pltpu.VMEM((blocks, w_count, ct, block), BF16),
            pltpu.VMEM((per_dev, toks, block), F32),
            pltpu.VMEM((chunks, w_count, ct, lat_dev), BF16),
            pltpu.VMEM((chunks, w_count, ct, lat_dev), BF16),
            pltpu.VMEM(targets.shape, BF16),
            pltpu.VMEM((slots + 1, rows, width), F32),
        ] + [pltpu.VMEM(b_piece_shape, BF16)] * 5 + [
            pltpu.VMEM(x_shape, BF16),
            pltpu.VMEM(x_shape, BF16),
            pltpu.VMEM((slots + 1, ct, block), F32),
            pltpu.VMEM((chunks, blocks, ct, block), BF16),
        ] + [pltpu.VMEM(z_piece_shape, BF16)] * 4 + [
            pltpu.VMEM((chunks, ct, columns), BF16),
            dma((slots,)), dma((chunks * w_count,)), dma((chunks * w_count,)),
        ] + [dma((chunks * n,))] * 3 + [dma((chunks * n * w_count,))] * 2 + [dma((b_pieces,))] * 4
        + [dma((x_sems,))] * 2 + [dma((z_pieces,))] * 4 + [
            dma((2 + w_count,)), dma((2 + w_count,)), dma((chunks,)), dma((chunks,)), dma((2 + w_count,)),
            dma((1 + lat_dev // wide,)),
        ],
        compiler_params=pltpu.CompilerParams(
            collective_id=cid, has_side_effects=True, vmem_limit_bytes=67043328
        ),
        name="step",
    )(dec_list, acts, enc_weight, enc_bias, gate, dec_weight, targets)


def decoder_grads(tables, lat, err, slots):
    layers, toks, width = err.shape
    blocks, _, half = lat.shape
    g = group_of(slots)
    at = Tables(slots, layers, blocks)

    def body(tab, l_ref, e_ref, o_ref):
        for i in range(g):
            k = pl.program_id(0) * g + i

            @pl.when(tab[at.raw + k] >= 0)
            def _():
                o_ref[i] = lax.dot_general(
                    l_ref[tab[at.id + k]], e_ref[tab[at.tgt + k]], (((0,), (0,)), ((), ())),
                    preferred_element_type=F32,
                )

            @pl.when(tab[at.raw + k] < 0)
            def _():
                o_ref[i] = jnp.zeros_like(o_ref[i])

    return slot_call(
        body, (tables,), (lat, err),
        [pl.BlockSpec((blocks, toks, half), lambda k, t: (0, 0, 0)),
         pl.BlockSpec((layers, toks, width), lambda k, t: (0, 0, 0))],
        jax.ShapeDtypeStruct((slots, half, width), F32),
        pl.BlockSpec((g, half, width), lambda k, t: (k, 0, 0)),
        [], 2 * slots * toks * half * width, "decoder_grads", slots // g,
    )


def local(acts, targets, enc_weight, enc_bias, gate_mask, dec_list, dec_weight):
    layers, tok_rows, width = acts.shape
    lat_dev = enc_weight.shape[1]
    slots, block, _ = dec_weight.shape
    w_count, r_count = lax.axis_size("wid"), lax.axis_size("rep")
    shape = (layers, w_count, tok_rows // w_count, width)
    scale = float(tok_rows * r_count) ** (-0.5)
    tables, pre_mine, lat, err, acts_all = step(
        acts.reshape(shape), enc_weight, enc_bias.reshape(1, lat_dev), gate_mask.T, dec_list.T,
        dec_weight, targets.reshape(shape), scale, 0,
    )
    pre_all = [pre_mine] + [
        lax.ppermute(pre_mine, "wid", [(i, (i - d) % w_count) for i in range(w_count)])
        for d in range(1, w_count)
    ]
    everyone = r_count * tok_rows
    dec_out = decoder_grads(
        tables, lat.reshape(lat.shape[0], everyone, block // r_count), err.reshape(layers, everyone, width),
        slots,
    )
    pre_all = jnp.stack(pre_all).reshape(everyone, lat_dev // r_count)
    enc_out = lax.dot_general(
        acts_all.reshape(everyone, width), pre_all, (((0,), (0,)), ((), ())), preferred_element_type=F32
    )
    bias_out = jnp.sum(pre_all.astype(F32), axis=0)
    return (enc_out, bias_out, dec_out)


def solution(mesh):
    return jax.shard_map(
        local,
        mesh=mesh,
        in_specs=(
            P(None, ("grp", "rep"), "wid"),
            P(None, ("grp", "rep"), "wid"),
            P("wid", "lay"),
            P("lay"),
            P(("grp", "rep"), "lay"),
            P("lay", None),
            P("lay", None, "wid"),
        ),
        out_specs=(
            P(("grp", "wid"), ("lay", "rep")),
            P(("grp", "lay", "rep")),
            P(("grp", "lay"), "rep", "wid"),
        ),
        check_vma=False,
    )
```

```python
import jax
import jax.numpy as jnp
from jax import lax
from jax.experimental import pallas as pl
from jax.experimental.pallas import tpu as pltpu
from jax.sharding import PartitionSpec as P

ROOT = 0.7978845608028654
CUBIC = 0.044715
MESH = pl.DeviceIdType.MESH
BF16 = jnp.bfloat16
F32 = jnp.float32
CHUNKS = 4
CUTS = 2
SKEW = 4
Z_SKEW = 4
P_PERIOD = 5
A_PERIOD = 9
B_PERIOD = 9
C_PERIOD = 7
A_GATE = 9
A_SKEW = 4
A_ACROSS = 6
B_ACROSS = 0
C_ACROSS = 3


def smooth_gate(shifted):
    inside_arg = ROOT * (shifted + CUBIC * shifted * shifted * shifted)
    return 0.5 * shifted * (1.0 + jnp.tanh(inside_arg))


def gate_slope(shifted):
    inside_arg = ROOT * (shifted + CUBIC * shifted * shifted * shifted)
    tanh_part = jnp.tanh(inside_arg)
    return 0.5 * (1.0 + tanh_part) + 0.5 * shifted * (1.0 - tanh_part * tanh_part) * ROOT * (
        1.0 + 3.0 * CUBIC * shifted * shifted
    )


def loop(first, count, step):
    if count <= 4:
        for d in range(first, count):
            step(d)
    else:
        lax.fori_loop(first, count, lambda d, c: (step(d), c)[1], 0)


def others(me, count, step):
    loop(1, count, lambda d: step(lax.rem(me + d, count)))


def signal(barrier, **where):
    pl.semaphore_signal(barrier, inc=1, device_id=where, device_id_type=MESH)


def remote(src, dst, send_sem, recv_sem, **where):
    return pltpu.make_async_remote_copy(
        src_ref=src, dst_ref=dst, send_sem=send_sem, recv_sem=recv_sem, device_id=where,
        device_id_type=MESH,
    )


ANY = pl.BlockSpec(memory_space=pl.ANY)


def nearest(l, n, d, step):
    for j in (l - d, l + d):

        @pl.when((j >= 0) & (j < n))
        def _():
            step(j)


def group_of(slots):
    return 3 if slots % 3 == 0 else 1


def slot_call(body, tables, args, in_specs, out_shape, out_spec, scratch, flops, name, grid):
    moved = sum(a.size * a.dtype.itemsize for a in args) + out_shape.size * out_shape.dtype.itemsize
    return pl.pallas_call(
        body,
        out_shape=out_shape,
        grid_spec=pltpu.PrefetchScalarGridSpec(
            num_scalar_prefetch=len(tables), grid=(grid,), in_specs=in_specs,
            out_specs=out_spec, scratch_shapes=scratch,
        ),
        compiler_params=pltpu.CompilerParams(vmem_limit_bytes=62 * 1024 * 1024),
        cost_estimate=pl.CostEstimate(flops=flops, bytes_accessed=moved, transcendentals=0),
        name=name,
    )(*tables, *args)


class Tables:
    def __init__(self, slots, layers, blocks):
        self.tgt, self.id, self.raw = 0, slots, 2 * slots
        self.prev_tgt, self.prev_id = 3 * slots, 4 * slots
        self.last_tgt = 5 * slots
        self.last_id = self.last_tgt + layers
        self.size = -(-(self.last_id + blocks) // 128) * 128


def chunk_count(toks):
    return next(c for c in (CHUNKS, 4, 2, 1) if toks % (16 * c) == 0 or c == 1)


def step(acts, enc_weight, enc_bias, gate, dec_list, dec_weight, targets, scale, cid):
    layers, w_count, toks, width = acts.shape
    lat_dev = enc_weight.shape[1]
    slots, block, _ = dec_weight.shape
    per_dev = lat_dev // block
    n, r_count = lax.axis_size("lay"), lax.axis_size("rep")
    assert r_count == 2
    blocks = n * per_dev
    blocks_layer = blocks // layers
    columns = lat_dev // r_count
    half = block // r_count
    at = Tables(slots, layers, blocks)
    chunks = chunk_count(toks)
    ct = toks // chunks
    rows = w_count * ct
    wide = min(lat_dev, 512)
    cols = lat_dev // wide

    cuts = next(c for c in (CUTS, 1) if width % (128 * c) == 0)
    part = width // cuts
    b_steps = layers * cuts
    b_pieces = chunks * b_steps

    split = 2 if per_dev % 2 == 0 else 1
    pb = per_dev // split
    z_steps = (n - 1) * split
    z_pieces = chunks * z_steps
    g = group_of(slots)
    groups = slots // g

    p_period, a_period = P_PERIOD, A_PERIOD
    b_period, c_period = max(b_steps, B_PERIOD), max(z_steps, C_PERIOD)
    per_step = -(-slots // b_period)
    a_decode = A_GATE + A_SKEW * (n - 1) + A_ACROSS + max(0, a_period - b_period) * (chunks - 1)
    b_first = a_decode + b_period
    c_slots = b_first + b_steps - 1 + SKEW * (n - 1) + B_ACROSS + max(0, b_period - c_period) * (chunks - 1)
    c_gather = c_slots + c_period + C_ACROSS
    ticks = c_gather + (chunks - 1) * c_period + split + (n - 1) * max(split, Z_SKEW)
    table_slots = -(-slots // (a_decode - 1))
    table_blocks = -(-blocks // (a_decode - 1))

    def body(d_ref, a_hbm, ew_hbm, b_ref, g_ref, w_hbm, t_hbm,
             tab, po_ref, lo_ref, eo_ref, ao_ref,
             a_ref, ew_ref, keep_ref, t_ref, w_ref, lat_ref, lat_now, sl_ref, p_out, p_in, e_ref, sums, own_ref, bu_in, bd_in, bu_out, bd_out,
             x_out, x_in, c_sums, made, zu_in, zd_in, zu_out, zd_out, twin_out,
             wsem, ps, pr, aus, ads, azr, axs, axr, bus, bur, bds, bdr, xs, xr, zus, zur, zds, zdr,
             ts, tr, tps, tpr, asem, isem):
        l, w, r = lax.axis_index("lay"), lax.axis_index("wid"), lax.axis_index("rep")
        twin = 1 - r

        def weight(k):
            return pltpu.make_async_copy(w_hbm.at[k], w_ref.at[k], wsem.at[k])

        layer = l * per_dev // blocks_layer
        acts_in = pltpu.make_async_copy(a_hbm.at[layer], a_ref, isem.at[0])
        enc_in = [
            pltpu.make_async_copy(ew_hbm.at[:, o:o + wide], ew_ref.at[:, o:o + wide], isem.at[1 + i])
            for i, o in enumerate(range(0, lat_dev, wide))
        ]
        acts_in.start()
        for copy in enc_in:
            copy.start()
        aims = pltpu.make_async_copy(t_hbm, t_ref, isem.at[1 + lat_dev // wide])
        loop(0, slots, lambda k: weight(k).start())
        aims.start()
        barrier = pltpu.get_barrier_semaphore()
        others(l, n, lambda j: signal(barrier, lay=j))
        others(w, w_count, lambda v: signal(barrier, wid=v))
        signal(barrier, rep=twin)
        sums[0] = jnp.zeros_like(sums[0])
        c_sums[0] = jnp.zeros_like(c_sums[0])
        keep_ref[...] = g_ref[...].astype(F32).T

        def listed(k, carry):
            t = d_ref[1, k]
            raw = jnp.where(t >= 0, d_ref[0, k] * blocks_layer + d_ref[2, k], -1)
            tab[at.tgt + k] = jnp.maximum(t, 0)
            tab[at.raw + k] = raw
            tab[at.id + k] = jnp.maximum(raw, 0)
            return carry

        lax.fori_loop(0, slots, listed, 0)

        def last_of(which, value, below):
            found = jnp.int32(0)
            for j in range(slots):
                found = jnp.where((which(j) == value) & (j < below), j + 1, found)
            return found

        def target(j):
            return d_ref[1, j]

        def named(j):
            return tab[at.raw + j]

        for t in range(layers):
            tab[at.last_tgt + t] = last_of(target, t, slots)

        def some_tables(s):
            for d in range(table_slots):
                k = s * table_slots + d

                @pl.when(k < slots)
                def _():
                    tab[at.prev_tgt + k] = last_of(target, target(k), k)
                    tab[at.prev_id + k] = last_of(named, named(k), k)

            for d in range(table_blocks):
                b = s * table_blocks + d

                @pl.when(b < blocks)
                def _():
                    tab[at.last_id + b] = last_of(named, b, slots)

        pl.semaphore_wait(barrier, n + w_count - 1)
        acts_in.wait()

        def chunk(c):
            return pl.ds(pl.multiple_of(c * ct, ct), ct)

        def at_chunk(s, first, period, do):
            t = s - first

            @pl.when((t >= 0) & (t < chunks * period))
            def _():
                @pl.when(lax.rem(t, period) == 0)
                def _():
                    do(t // period)


        def p_send(c, i, v):
            over, q = pl.ds(i * wide, wide), (c * cols + i) * w_count
            return remote(p_out.at[c, v, :, over], p_in.at[c, w, :, over], ps.at[q + v], pr.at[q + w], wid=v)

        def p_landed(c, i, v):
            over, q = pl.ds(i * wide, wide), (c * cols + i) * w_count
            return remote(p_in.at[c, v, :, over], p_in.at[c, v, :, over], ps.at[q + v], pr.at[q + v], wid=v)

        def product(c):
            held = a_ref[:, chunk(c), :].reshape(rows, width)
            for i in range(cols):
                @pl.when(c == 0)
                def _():
                    enc_in[i].wait()

                over = slice(i * wide, (i + 1) * wide)
                made_here = jnp.dot(held, ew_ref[:, over], preferred_element_type=F32).astype(BF16)
                for v in range(w_count):
                    p_out[c, v, :, over] = made_here[v * ct:(v + 1) * ct]
                others(w, w_count, lambda v: p_send(c, i, v).start())

        def shard(c, j, v):
            return lat_ref.at[pl.ds(j * per_dev, per_dev), v, chunk(c)]

        def a_up(c, j):
            return remote(shard(c, j, w), shard(c, j, w), aus.at[c * n + j], azr.at[c * n + j], lay=l + 1)

        def a_dn(c, j):
            return remote(shard(c, j, w), shard(c, j, w), ads.at[c * n + j], azr.at[c * n + j], lay=l - 1)

        def across(c, j, v, source):
            return remote(shard(c, j, source), shard(c, j, source), axs.at[(c * n + j) * w_count + v],
                          axr.at[(c * n + j) * w_count + source], wid=v)

        def goes(c, j, do):
            @pl.when((j <= l) & (l < n - 1))
            def _():
                do(a_up(c, j))

            @pl.when((j >= l) & (l > 0))
            def _():
                do(a_dn(c, j))

            others(w, w_count, lambda v: do(across(c, j, v, w)))

        def gated(c):
            for i in range(cols):
                others(w, w_count, lambda v: p_landed(c, i, v).wait_recv())
            keep = keep_ref[pl.ds(pl.multiple_of(w * toks + c * ct, ct), ct), :]
            for b in range(per_dev):
                over = slice(b * block, (b + 1) * block)
                shifted = p_out[c, w, :, over].astype(F32) + b_ref[:, over]
                for d in range(1, w_count):
                    shifted = shifted + p_in[c, lax.rem(w + d, w_count), :, over].astype(F32)
                held = keep[:, b:b + 1]
                lat_ref[l * per_dev + b, w, chunk(c), :] = (smooth_gate(shifted) * held).astype(BF16)
                sl_ref[b, chunk(c), :] = gate_slope(shifted) * held
            goes(c, l, lambda copy: copy.start())

        def take(c, j):
            remote(shard(c, j, w), shard(c, j, w), aus.at[c * n + j], azr.at[c * n + j], lay=j).wait_recv()
            goes(c, j, lambda copy: copy.start())

        def crossed(c):
            loop(0, n, lambda j: others(w, w_count, lambda v: across(c, j, v, v).wait_recv()))
            lat_now[...] = lat_ref[:, :, chunk(c), :]


        def slot(k):
            held = lat_now[tab[at.id + k]].reshape(rows, block)
            sums[k + 1] = jnp.dot(held, w_ref[k], preferred_element_type=F32) + sums[tab[at.prev_tgt + k]]

        def emit(c):
            for t in range(layers):
                total = sums[tab[at.last_tgt + t]].astype(BF16)
                for i in range(cuts):
                    own_ref[c * b_steps + t * cuts + i] = total[:, i * part:(i + 1) * part]

        def b_up(q):
            return remote(bu_out.at[q], bu_in.at[q], bus.at[q], bur.at[q], lay=l + 1)

        def b_dn(q):
            return remote(bd_out.at[q], bd_in.at[q], bds.at[q], bdr.at[q], lay=l - 1)

        def b_inside(q):
            return (q >= 0) & (q < chunks * b_period) & (lax.rem(q + b_period * chunks, b_period) < b_steps)

        def b_piece(q):
            return q // b_period * b_steps + lax.rem(q + b_period * chunks, b_period)

        def hand_on(s):
            q, p = s - SKEW * l, s - SKEW * (n - 1 - l)
            e = s - SKEW * jnp.maximum(l, n - 1 - l)
            q_in, p_in_, e_in = b_inside(q), b_inside(p), b_inside(e)
            q, p, e = b_piece(q), b_piece(p), b_piece(e)

            @pl.when(q_in & (l > 0))
            def _():
                remote(bu_in.at[q], bu_in.at[q], bus.at[q], bur.at[q], lay=l).wait_recv()

            @pl.when(q_in & (l == 0))
            def _():
                bu_out[q] = own_ref[q]

            @pl.when(q_in & (l > 0) & (l < n - 1))
            def _():
                bu_out[q] = (own_ref[q].astype(F32) + bu_in[q].astype(F32)).astype(BF16)

            @pl.when(p_in_ & (l < n - 1))
            def _():
                remote(bd_in.at[p], bd_in.at[p], bds.at[p], bdr.at[p], lay=l).wait_recv()

            @pl.when(p_in_ & (l == n - 1))
            def _():
                bd_out[p] = own_ref[p]

            @pl.when(p_in_ & (l > 0) & (l < n - 1))
            def _():
                bd_out[p] = (own_ref[p].astype(F32) + bd_in[p].astype(F32)).astype(BF16)

            def error(total):
                c, i = e // b_steps, lax.rem(e, b_steps)
                t, i = i // cuts, lax.rem(i, cuts)
                over = pl.ds(pl.multiple_of(i * part, part), part)
                aim = t_ref[t, :, chunk(c), over].reshape(rows, part).astype(F32)
                e_ref[t, :, chunk(c), over] = ((total - aim) * scale).astype(BF16).reshape(w_count, ct, part)

            @pl.when(e_in & (l == 0))
            def _():
                error(own_ref[e].astype(F32) + bd_in[e].astype(F32))

            @pl.when(e_in & (l == n - 1))
            def _():
                error(own_ref[e].astype(F32) + bu_in[e].astype(F32))

            @pl.when(e_in & (l > 0) & (l < n - 1))
            def _():
                error(own_ref[e].astype(F32) + bu_in[e].astype(F32) + bd_in[e].astype(F32))

            @pl.when(q_in & (l < n - 1))
            def _():
                b_up(q).start()

            @pl.when(p_in_ & (l > 0))
            def _():
                b_dn(p).start()


        def x_send(c, i, v):
            where = pl.ds(i * g, g)
            return remote(x_out.at[c, v, where], x_in.at[c, w, where], xs.at[(c * groups + i) * w_count + v],
                          xr.at[(c * groups + i) * w_count + w], wid=v)

        def x_landed(c, i, v):
            where = pl.ds(i * g, g)
            return remote(x_in.at[c, v, where], x_in.at[c, v, where],
                          xs.at[(c * groups + i) * w_count + v],
                          xr.at[(c * groups + i) * w_count + v], wid=v)

        def slot_group(c, i):
            for k in [i * g + d for d in range(g)]:
                held = e_ref[tab[at.tgt + k], :, chunk(c), :].reshape(rows, width)
                back = lax.dot_general(
                    held, w_ref[k], (((1,), (1,)), ((), ())), preferred_element_type=F32
                ).astype(BF16).reshape(w_count, ct, block)
                for v in range(w_count):
                    x_out[c, v, k] = back[v]
            others(w, w_count, lambda v: x_send(c, i, v).start())

        def gather(c):
            def landed(i, carry):
                others(w, w_count, lambda v: x_landed(c, i, v).wait_recv())
                return carry

            lax.fori_loop(0, groups, landed, 0)

            def one(k, carry):
                total = c_sums[tab[at.prev_id + k]] + x_out[c, w, k].astype(F32)
                for d in range(1, w_count):
                    total = total + x_in[c, lax.rem(w + d, w_count), k].astype(F32)
                c_sums[k + 1] = total
                return carry

            lax.fori_loop(0, slots, one, 0)

            def out(b, carry):
                made[c, b] = c_sums[tab[at.last_id + b]].astype(BF16)
                return carry

            lax.fori_loop(0, blocks, out, 0)

        def z_up(q):
            return remote(zu_out.at[q], zu_in.at[q], zus.at[q], zur.at[q], lay=l + 1)

        def z_dn(q):
            return remote(zd_out.at[q], zd_in.at[q], zds.at[q], zdr.at[q], lay=l - 1)

        def z_inside(q):
            return (q >= 0) & (q < chunks * c_period) & (lax.rem(q + c_period * chunks, c_period) < z_steps)

        def z_piece(q):
            return q // c_period * z_steps + lax.rem(q + c_period * chunks, c_period)

        def own_z(q, dest):
            return made[q // z_steps, pl.ds(dest * per_dev + lax.rem(q, split) * pb, pb)].astype(F32)

        def twin_pre(c):
            return remote(twin_out.at[c], po_ref.at[r, chunk(c)], tps.at[c], tpr.at[c], rep=twin)

        def twin_landed(c):
            return remote(twin_out.at[c], po_ref.at[twin, chunk(c)], tps.at[c], tpr.at[c], rep=twin)

        def reduce_on(s):
            q, p = s - Z_SKEW * l, s - Z_SKEW * (n - 1 - l)
            q_in, p_in_ = z_inside(q), z_inside(p)
            q, p = z_piece(q), z_piece(p)
            to_up = n - 1 - lax.rem(q + z_pieces, z_steps) // split
            to_dn = lax.rem(p + z_pieces, z_steps) // split

            @pl.when(q_in & (l > 0) & (to_up >= l))
            def _():
                remote(zu_in.at[q], zu_in.at[q], zus.at[q], zur.at[q], lay=l).wait_recv()

            @pl.when(q_in & (l == 0))
            def _():
                zu_out[q] = own_z(q, to_up).astype(BF16)

            @pl.when(q_in & (l > 0) & (to_up > l))
            def _():
                zu_out[q] = (own_z(q, to_up) + zu_in[q].astype(F32)).astype(BF16)

            @pl.when(p_in_ & (l < n - 1) & (to_dn <= l))
            def _():
                remote(zd_in.at[p], zd_in.at[p], zds.at[p], zdr.at[p], lay=l).wait_recv()

            @pl.when(p_in_ & (l == n - 1))
            def _():
                zd_out[p] = own_z(p, to_dn).astype(BF16)

            @pl.when(p_in_ & (l < n - 1) & (to_dn < l))
            def _():
                zd_out[p] = (own_z(p, to_dn) + zd_in[p].astype(F32)).astype(BF16)

            off_up = (n - 1 - l) * split
            off_dn = l * split
            f = s - jnp.maximum(off_up + Z_SKEW * l, off_dn + Z_SKEW * (n - 1 - l))
            i = lax.rem(f + c_period * chunks, c_period)
            whole = (f >= 0) & (f < chunks * c_period) & (i < split)
            c = f // c_period

            def finish(total):
                blocks_here = pl.ds(i * pb, pb)
                grad = (total * sl_ref[blocks_here, chunk(c), :]).astype(BF16)
                if split == r_count:
                    @pl.when(i == r)
                    def _():
                        for b in range(pb):
                            po_ref[r, chunk(c), b * block:(b + 1) * block] = grad[b]

                    @pl.when(i != r)
                    def _():
                        for b in range(pb):
                            twin_out[c, :, b * block:(b + 1) * block] = grad[b]
                else:
                    for b in range(pb):
                        for side in range(r_count):
                            cut = grad[b][:, side * half:(side + 1) * half]

                            @pl.when(r == side)
                            def _():
                                po_ref[side, chunk(c), b * half:(b + 1) * half] = cut

                            @pl.when(r != side)
                            def _():
                                twin_out[c, :, b * half:(b + 1) * half] = cut

            def mid():
                return made[c, pl.ds(l * per_dev + i * pb, pb)].astype(F32)

            @pl.when(whole & (l == 0))
            def _():
                finish(mid() + zd_in[c * z_steps + off_dn + i].astype(F32))

            @pl.when(whole & (l == n - 1))
            def _():
                finish(mid() + zu_in[c * z_steps + off_up + i].astype(F32))

            @pl.when(whole & (l > 0) & (l < n - 1))
            def _():
                finish(mid() + zu_in[c * z_steps + off_up + i].astype(F32)
                       + zd_in[c * z_steps + off_dn + i].astype(F32))

            @pl.when(q_in & (to_up > l))
            def _():
                z_up(q).start()

            @pl.when(p_in_ & (to_dn < l))
            def _():
                z_dn(p).start()

            @pl.when(whole & (i == split - 1))
            def _():
                twin_pre(c).start()


        twins = [
            remote(lat_ref.at[:, :, :, pl.ds(pl.multiple_of(twin * half, half), half)], lo_ref.at[:, r],
                   ts.at[0], tr.at[0], rep=twin),
            remote(e_ref, eo_ref.at[:, r], ts.at[1], tr.at[1], rep=twin),
        ] + [
            remote(a_ref.at[v], ao_ref.at[lax.rem(v - w + w_count, w_count), r], ts.at[2 + v], tr.at[2 + v],
                   rep=twin)
            for v in range(w_count)
        ]
        mine = [
            pltpu.make_async_copy(
                lat_ref.at[:, :, :, pl.ds(pl.multiple_of(r * half, half), half)], lo_ref.at[:, r], asem.at[0]),
            pltpu.make_async_copy(e_ref, eo_ref.at[:, r], asem.at[1]),
        ] + [
            pltpu.make_async_copy(
                a_ref.at[v], ao_ref.at[lax.rem(v - w + w_count, w_count), r], asem.at[2 + v])
            for v in range(w_count)
        ]

        def tick(s, carry):
            def arrive(d):
                at_chunk(s, A_GATE + A_SKEW * d, a_period, lambda c: nearest(l, n, d, lambda j: take(c, j)))

            loop(1, n, arrive)
            hand_on(s - b_first)
            at_chunk(s, c_gather, c_period, gather)
            reduce_on(s - c_gather)
            at_chunk(s, A_GATE, a_period, gated)
            at_chunk(s, 0, p_period, product)

            @pl.when(s < a_decode - 1)
            def _():
                some_tables(s)

            t = s - c_slots

            @pl.when((t >= 0) & (t < chunks * c_period))
            def _():
                c, i = t // c_period, lax.rem(t, c_period)
                lax.fori_loop(
                    (i * groups + c_period - 1) // c_period, ((i + 1) * groups + c_period - 1) // c_period,
                    lambda j, z: (slot_group(c, j), z)[1], 0,
                )

            u = s - a_decode

            @pl.when((u >= 0) & (u < chunks * b_period))
            def _():
                c, i = u // b_period, lax.rem(u, b_period)

                @pl.when(i == 0)
                def _():
                    crossed(c)

                for d in range(per_step):
                    @pl.when(i * per_step + d < slots)
                    def _():
                        slot(i * per_step + d)

                @pl.when(i == b_period - 1)
                def _():
                    emit(c)

            @pl.when(s == a_decode - 1)
            def _():
                loop(0, slots, lambda k: weight(k).wait())
                aims.wait()
                for v in range(w_count):
                    twins[2 + v].start()
                    mine[2 + v].start()

            @pl.when(s == a_decode + (chunks - 1) * b_period)
            def _():
                twins[0].start()
                mine[0].start()

            @pl.when(s == c_slots + (chunks - 1) * c_period)
            def _():
                twins[1].start()
                mine[1].start()

            return carry

        lax.fori_loop(0, ticks, tick, 0)

        def a_sent(q, carry):
            goes(q // n, lax.rem(q, n), lambda copy: copy.wait_send())
            return carry

        lax.fori_loop(0, chunks * n, a_sent, 0)

        def b_sent(q, carry):
            @pl.when(l < n - 1)
            def _():
                b_up(q).wait_send()

            @pl.when(l > 0)
            def _():
                b_dn(q).wait_send()

            return carry

        lax.fori_loop(0, b_pieces, b_sent, 0)

        def z_sent(q, carry):
            to_up = n - 1 - lax.rem(q, z_steps) // split
            to_dn = lax.rem(q, z_steps) // split

            @pl.when(to_up > l)
            def _():
                z_up(q).wait_send()

            @pl.when(to_dn < l)
            def _():
                z_dn(q).wait_send()

            return carry

        lax.fori_loop(0, z_pieces, z_sent, 0)

        def x_sent(q, carry):
            others(w, w_count, lambda v: x_send(q // groups, lax.rem(q, groups), v).wait_send())
            return carry

        lax.fori_loop(0, chunks * groups, x_sent, 0)
        for c in range(chunks):
            for i in range(cols):
                others(w, w_count, lambda v: p_send(c, i, v).wait_send())
            twin_landed(c).wait()
        for copy in twins + mine:
            copy.wait()

    b_piece_shape = (b_pieces, rows, part)
    z_piece_shape = (z_pieces, pb, ct, block)
    x_shape = (chunks, w_count, slots, ct, block)
    lat_shape = (blocks, w_count, toks, block)
    vmem = pl.BlockSpec(memory_space=pltpu.VMEM)
    smem = pl.BlockSpec(memory_space=pltpu.SMEM)
    dma = pltpu.SemaphoreType.DMA
    x_sems = chunks * groups * w_count
    return pl.pallas_call(
        body,
        out_shape=(
            jax.ShapeDtypeStruct((at.size,), jnp.int32),
            jax.ShapeDtypeStruct((r_count, toks, columns), BF16),
            jax.ShapeDtypeStruct((blocks, r_count, w_count, toks, half), BF16),
            jax.ShapeDtypeStruct((layers, r_count, w_count, toks, width), BF16),
            jax.ShapeDtypeStruct((w_count, r_count, toks, width), BF16),
        ),
        in_specs=[smem, ANY, ANY, vmem, vmem, ANY, ANY],
        out_specs=(smem, vmem, ANY, ANY, ANY),
        scratch_shapes=[
            pltpu.VMEM((w_count, toks, width), BF16),
            pltpu.VMEM(enc_weight.shape, BF16),
            pltpu.VMEM((w_count * toks, per_dev), F32),
            pltpu.VMEM(targets.shape, BF16),
            pltpu.VMEM(dec_weight.shape, BF16),
            pltpu.VMEM(lat_shape, BF16),
            pltpu.VMEM((blocks, w_count, ct, block), BF16),
            pltpu.VMEM((per_dev, toks, block), F32),
            pltpu.VMEM((chunks, w_count, ct, lat_dev), BF16),
            pltpu.VMEM((chunks, w_count, ct, lat_dev), BF16),
            pltpu.VMEM(targets.shape, BF16),
            pltpu.VMEM((slots + 1, rows, width), F32),
        ] + [pltpu.VMEM(b_piece_shape, BF16)] * 5 + [
            pltpu.VMEM(x_shape, BF16),
            pltpu.VMEM(x_shape, BF16),
            pltpu.VMEM((slots + 1, ct, block), F32),
            pltpu.VMEM((chunks, blocks, ct, block), BF16),
        ] + [pltpu.VMEM(z_piece_shape, BF16)] * 4 + [
            pltpu.VMEM((chunks, ct, columns), BF16),
            dma((slots,)), dma((chunks * cols * w_count,)), dma((chunks * cols * w_count,)),
        ] + [dma((chunks * n,))] * 3 + [dma((chunks * n * w_count,))] * 2 + [dma((b_pieces,))] * 4
        + [dma((x_sems,))] * 2 + [dma((z_pieces,))] * 4 + [
            dma((2 + w_count,)), dma((2 + w_count,)), dma((chunks,)), dma((chunks,)), dma((2 + w_count,)),
            dma((2 + lat_dev // wide,)),
        ],
        compiler_params=pltpu.CompilerParams(
            collective_id=cid, has_side_effects=True, vmem_limit_bytes=67043328
        ),
        name="step",
    )(dec_list, acts, enc_weight, enc_bias, gate, dec_weight, targets)


def decoder_grads(tables, lat, err, slots):
    layers, toks, width = err.shape
    blocks, _, half = lat.shape
    g = group_of(slots)
    at = Tables(slots, layers, blocks)

    def body(tab, l_ref, e_ref, o_ref):
        for i in range(g):
            k = pl.program_id(0) * g + i

            @pl.when(tab[at.raw + k] >= 0)
            def _():
                o_ref[i] = lax.dot_general(
                    l_ref[tab[at.id + k]], e_ref[tab[at.tgt + k]], (((0,), (0,)), ((), ())),
                    preferred_element_type=F32,
                )

            @pl.when(tab[at.raw + k] < 0)
            def _():
                o_ref[i] = jnp.zeros_like(o_ref[i])

    return slot_call(
        body, (tables,), (lat, err),
        [pl.BlockSpec((blocks, toks, half), lambda k, t: (0, 0, 0)),
         pl.BlockSpec((layers, toks, width), lambda k, t: (0, 0, 0))],
        jax.ShapeDtypeStruct((slots, half, width), F32),
        pl.BlockSpec((g, half, width), lambda k, t: (k, 0, 0)),
        [], 2 * slots * toks * half * width, "decoder_grads", slots // g,
    )


def local(acts, targets, enc_weight, enc_bias, gate_mask, dec_list, dec_weight):
    layers, tok_rows, width = acts.shape
    lat_dev = enc_weight.shape[1]
    slots, block, _ = dec_weight.shape
    w_count, r_count = lax.axis_size("wid"), lax.axis_size("rep")
    shape = (layers, w_count, tok_rows // w_count, width)
    scale = float(tok_rows * r_count) ** (-0.5)
    tables, pre_mine, lat, err, acts_all = step(
        acts.reshape(shape), enc_weight, enc_bias.reshape(1, lat_dev), gate_mask.T, dec_list.T,
        dec_weight, targets.reshape(shape), scale, 0,
    )
    pre_all = [pre_mine] + [
        lax.ppermute(pre_mine, "wid", [(i, (i - d) % w_count) for i in range(w_count)])
        for d in range(1, w_count)
    ]
    everyone = r_count * tok_rows
    dec_out = decoder_grads(
        tables, lat.reshape(lat.shape[0], everyone, block // r_count), err.reshape(layers, everyone, width),
        slots,
    )
    pre_all = jnp.stack(pre_all).reshape(everyone, lat_dev // r_count)
    enc_out = lax.dot_general(
        acts_all.reshape(everyone, width), pre_all, (((0,), (0,)), ((), ())), preferred_element_type=F32
    )
    bias_out = jnp.sum(pre_all.astype(F32), axis=0)
    return (enc_out, bias_out, dec_out)


def solution(mesh):
    return jax.shard_map(
        local,
        mesh=mesh,
        in_specs=(
            P(None, ("grp", "rep"), "wid"),
            P(None, ("grp", "rep"), "wid"),
            P("wid", "lay"),
            P("lay"),
            P(("grp", "rep"), "lay"),
            P("lay", None),
            P("lay", None, "wid"),
        ),
        out_specs=(
            P(("grp", "wid"), ("lay", "rep")),
            P(("grp", "lay", "rep")),
            P(("grp", "lay"), "rep", "wid"),
        ),
        check_vma=False,
    )
```

```python
import jax
import jax.numpy as jnp
from jax import lax
from jax.experimental import pallas as pl
from jax.experimental.pallas import tpu as pltpu
from jax.sharding import PartitionSpec as P

ROOT = 0.7978845608028654
CUBIC = 0.044715
MESH = pl.DeviceIdType.MESH
BF16 = jnp.bfloat16
F32 = jnp.float32
CHUNKS = 4
CUTS = 2
SKEW = 4
Z_SKEW = 4
P_PERIOD = 5
A_PERIOD = 9
B_PERIOD = 8
C_PERIOD = 7
A_GATE = 9
A_SKEW = 4
A_ACROSS = 4
B_ACROSS = 0
C_ACROSS = 2


def smooth_gate(shifted):
    inside_arg = ROOT * (shifted + CUBIC * shifted * shifted * shifted)
    return 0.5 * shifted * (1.0 + jnp.tanh(inside_arg))


def gate_slope(shifted):
    inside_arg = ROOT * (shifted + CUBIC * shifted * shifted * shifted)
    tanh_part = jnp.tanh(inside_arg)
    return 0.5 * (1.0 + tanh_part) + 0.5 * shifted * (1.0 - tanh_part * tanh_part) * ROOT * (
        1.0 + 3.0 * CUBIC * shifted * shifted
    )


def loop(first, count, step):
    if count <= 4:
        for d in range(first, count):
            step(d)
    else:
        lax.fori_loop(first, count, lambda d, c: (step(d), c)[1], 0)


def others(me, count, step):
    loop(1, count, lambda d: step(lax.rem(me + d, count)))


def signal(barrier, **where):
    pl.semaphore_signal(barrier, inc=1, device_id=where, device_id_type=MESH)


def remote(src, dst, send_sem, recv_sem, **where):
    return pltpu.make_async_remote_copy(
        src_ref=src, dst_ref=dst, send_sem=send_sem, recv_sem=recv_sem, device_id=where,
        device_id_type=MESH,
    )


ANY = pl.BlockSpec(memory_space=pl.ANY)


def nearest(l, n, d, step):
    for j in (l - d, l + d):

        @pl.when((j >= 0) & (j < n))
        def _():
            step(j)


def group_of(slots):
    return 3 if slots % 3 == 0 else 1


def slot_call(body, tables, args, in_specs, out_shape, out_spec, scratch, flops, name, grid):
    moved = sum(a.size * a.dtype.itemsize for a in args) + out_shape.size * out_shape.dtype.itemsize
    return pl.pallas_call(
        body,
        out_shape=out_shape,
        grid_spec=pltpu.PrefetchScalarGridSpec(
            num_scalar_prefetch=len(tables), grid=(grid,), in_specs=in_specs,
            out_specs=out_spec, scratch_shapes=scratch,
        ),
        compiler_params=pltpu.CompilerParams(vmem_limit_bytes=62 * 1024 * 1024),
        cost_estimate=pl.CostEstimate(flops=flops, bytes_accessed=moved, transcendentals=0),
        name=name,
    )(*tables, *args)


class Tables:
    def __init__(self, slots, layers, blocks):
        self.tgt, self.id, self.raw = 0, slots, 2 * slots
        self.prev_tgt, self.prev_id = 3 * slots, 4 * slots
        self.last_tgt = 5 * slots
        self.last_id = self.last_tgt + layers
        self.size = -(-(self.last_id + blocks) // 128) * 128


def chunk_count(toks):
    return next(c for c in (CHUNKS, 4, 2, 1) if toks % (16 * c) == 0 or c == 1)


def step(acts, enc_weight, enc_bias, gate, dec_list, dec_weight, targets, scale, cid):
    layers, w_count, toks, width = acts.shape
    lat_dev = enc_weight.shape[1]
    slots, block, _ = dec_weight.shape
    per_dev = lat_dev // block
    n, r_count = lax.axis_size("lay"), lax.axis_size("rep")
    assert r_count == 2
    blocks = n * per_dev
    blocks_layer = blocks // layers
    columns = lat_dev // r_count
    half = block // r_count
    at = Tables(slots, layers, blocks)
    chunks = chunk_count(toks)
    ct = toks // chunks
    rows = w_count * ct
    wide = min(lat_dev, 512)
    cols = lat_dev // wide

    cuts = next(c for c in (CUTS, 1) if width % (128 * c) == 0)
    part = width // cuts
    b_steps = layers * cuts
    b_pieces = chunks * b_steps

    split = 2 if per_dev % 2 == 0 else 1
    pb = per_dev // split
    z_steps = (n - 1) * split
    z_pieces = chunks * z_steps
    g = group_of(slots)
    groups = slots // g

    p_period, a_period = P_PERIOD, A_PERIOD
    b_period, c_period = max(b_steps, B_PERIOD), max(z_steps, C_PERIOD)
    per_step = -(-slots // b_period)
    a_decode = A_GATE + A_SKEW * (n - 1) + A_ACROSS + max(0, a_period - b_period) * (chunks - 1)
    b_first = a_decode + b_period
    c_slots = b_first + b_steps - 1 + SKEW * (n - 1) + B_ACROSS + max(0, b_period - c_period) * (chunks - 1)
    c_gather = c_slots + c_period + C_ACROSS
    ticks = c_gather + (chunks - 1) * c_period + split + (n - 1) * max(split, Z_SKEW)
    table_slots = -(-slots // (a_decode - 1))
    table_blocks = -(-blocks // (a_decode - 1))

    def body(d_ref, a_hbm, ew_hbm, b_ref, g_ref, w_hbm, t_hbm,
             tab, po_ref, lo_ref, eo_ref, ao_ref,
             a_ref, ew_ref, keep_ref, t_ref, w_ref, lat_ref, lat_now, sl_ref, p_out, p_in, e_ref, sums, own_ref, bu_in, bd_in, bu_out, bd_out,
             x_out, x_in, c_sums, made, zu_in, zd_in, zu_out, zd_out, twin_out,
             wsem, ps, pr, aus, ads, azr, axs, axr, bus, bur, bds, bdr, xs, xr, zus, zur, zds, zdr,
             ts, tr, tps, tpr, asem, isem):
        l, w, r = lax.axis_index("lay"), lax.axis_index("wid"), lax.axis_index("rep")
        twin = 1 - r

        def weight(k):
            return pltpu.make_async_copy(w_hbm.at[k], w_ref.at[k], wsem.at[k])

        layer = l * per_dev // blocks_layer
        acts_in = pltpu.make_async_copy(a_hbm.at[layer], a_ref, isem.at[0])
        enc_in = [
            pltpu.make_async_copy(ew_hbm.at[:, o:o + wide], ew_ref.at[:, o:o + wide], isem.at[1 + i])
            for i, o in enumerate(range(0, lat_dev, wide))
        ]
        acts_in.start()
        for copy in enc_in:
            copy.start()
        aims = pltpu.make_async_copy(t_hbm, t_ref, isem.at[1 + lat_dev // wide])
        loop(0, slots, lambda k: weight(k).start())
        aims.start()
        barrier = pltpu.get_barrier_semaphore()
        others(l, n, lambda j: signal(barrier, lay=j))
        others(w, w_count, lambda v: signal(barrier, wid=v))
        signal(barrier, rep=twin)
        sums[0] = jnp.zeros_like(sums[0])
        c_sums[0] = jnp.zeros_like(c_sums[0])
        keep_ref[...] = g_ref[...].astype(F32).T

        def listed(k, carry):
            t = d_ref[1, k]
            raw = jnp.where(t >= 0, d_ref[0, k] * blocks_layer + d_ref[2, k], -1)
            tab[at.tgt + k] = jnp.maximum(t, 0)
            tab[at.raw + k] = raw
            tab[at.id + k] = jnp.maximum(raw, 0)
            return carry

        lax.fori_loop(0, slots, listed, 0)

        def last_of(which, value, below):
            found = jnp.int32(0)
            for j in range(slots):
                found = jnp.where((which(j) == value) & (j < below), j + 1, found)
            return found

        def target(j):
            return d_ref[1, j]

        def named(j):
            return tab[at.raw + j]

        for t in range(layers):
            tab[at.last_tgt + t] = last_of(target, t, slots)

        def some_tables(s):
            for d in range(table_slots):
                k = s * table_slots + d

                @pl.when(k < slots)
                def _():
                    tab[at.prev_tgt + k] = last_of(target, target(k), k)
                    tab[at.prev_id + k] = last_of(named, named(k), k)

            for d in range(table_blocks):
                b = s * table_blocks + d

                @pl.when(b < blocks)
                def _():
                    tab[at.last_id + b] = last_of(named, b, slots)

        pl.semaphore_wait(barrier, n + w_count - 1)
        acts_in.wait()

        def chunk(c):
            return pl.ds(pl.multiple_of(c * ct, ct), ct)

        def at_chunk(s, first, period, do):
            t = s - first

            @pl.when((t >= 0) & (t < chunks * period))
            def _():
                @pl.when(lax.rem(t, period) == 0)
                def _():
                    do(t // period)


        def p_send(c, i, v):
            over, q = pl.ds(i * wide, wide), (c * cols + i) * w_count
            return remote(p_out.at[c, v, :, over], p_in.at[c, w, :, over], ps.at[q + v], pr.at[q + w], wid=v)

        def p_landed(c, i, v):
            over, q = pl.ds(i * wide, wide), (c * cols + i) * w_count
            return remote(p_in.at[c, v, :, over], p_in.at[c, v, :, over], ps.at[q + v], pr.at[q + v], wid=v)

        def product(c):
            held = a_ref[:, chunk(c), :].reshape(rows, width)
            for i in range(cols):
                @pl.when(c == 0)
                def _():
                    enc_in[i].wait()

                over = slice(i * wide, (i + 1) * wide)
                made_here = jnp.dot(held, ew_ref[:, over], preferred_element_type=F32).astype(BF16)
                for v in range(w_count):
                    p_out[c, v, :, over] = made_here[v * ct:(v + 1) * ct]
                others(w, w_count, lambda v: p_send(c, i, v).start())

        def shard(c, j, v):
            return lat_ref.at[pl.ds(j * per_dev, per_dev), v, chunk(c)]

        def a_up(c, j):
            return remote(shard(c, j, w), shard(c, j, w), aus.at[c * n + j], azr.at[c * n + j], lay=l + 1)

        def a_dn(c, j):
            return remote(shard(c, j, w), shard(c, j, w), ads.at[c * n + j], azr.at[c * n + j], lay=l - 1)

        def across(c, j, v, source):
            return remote(shard(c, j, source), shard(c, j, source), axs.at[(c * n + j) * w_count + v],
                          axr.at[(c * n + j) * w_count + source], wid=v)

        def goes(c, j, do):
            @pl.when((j <= l) & (l < n - 1))
            def _():
                do(a_up(c, j))

            @pl.when((j >= l) & (l > 0))
            def _():
                do(a_dn(c, j))

            others(w, w_count, lambda v: do(across(c, j, v, w)))

        def gated(c):
            for i in range(cols):
                others(w, w_count, lambda v: p_landed(c, i, v).wait_recv())
            keep = keep_ref[pl.ds(pl.multiple_of(w * toks + c * ct, ct), ct), :]
            for b in range(per_dev):
                over = slice(b * block, (b + 1) * block)
                shifted = p_out[c, w, :, over].astype(F32) + b_ref[:, over]
                for d in range(1, w_count):
                    shifted = shifted + p_in[c, lax.rem(w + d, w_count), :, over].astype(F32)
                held = keep[:, b:b + 1]
                lat_ref[l * per_dev + b, w, chunk(c), :] = (smooth_gate(shifted) * held).astype(BF16)
                sl_ref[b, chunk(c), :] = gate_slope(shifted) * held
            goes(c, l, lambda copy: copy.start())

        def take(c, j):
            remote(shard(c, j, w), shard(c, j, w), aus.at[c * n + j], azr.at[c * n + j], lay=j).wait_recv()
            goes(c, j, lambda copy: copy.start())

        def crossed(c):
            loop(0, n, lambda j: others(w, w_count, lambda v: across(c, j, v, v).wait_recv()))
            lat_now[...] = lat_ref[:, :, chunk(c), :]


        def slot(k):
            held = lat_now[tab[at.id + k]].reshape(rows, block)
            sums[k + 1] = jnp.dot(held, w_ref[k], preferred_element_type=F32) + sums[tab[at.prev_tgt + k]]

        def emit(c):
            for t in range(layers):
                total = sums[tab[at.last_tgt + t]].astype(BF16)
                for i in range(cuts):
                    own_ref[c * b_steps + t * cuts + i] = total[:, i * part:(i + 1) * part]

        def b_up(q):
            return remote(bu_out.at[q], bu_in.at[q], bus.at[q], bur.at[q], lay=l + 1)

        def b_dn(q):
            return remote(bd_out.at[q], bd_in.at[q], bds.at[q], bdr.at[q], lay=l - 1)

        def b_inside(q):
            return (q >= 0) & (q < chunks * b_period) & (lax.rem(q + b_period * chunks, b_period) < b_steps)

        def b_piece(q):
            return q // b_period * b_steps + lax.rem(q + b_period * chunks, b_period)

        def hand_on(s):
            q, p = s - SKEW * l, s - SKEW * (n - 1 - l)
            e = s - SKEW * jnp.maximum(l, n - 1 - l)
            q_in, p_in_, e_in = b_inside(q), b_inside(p), b_inside(e)
            q, p, e = b_piece(q), b_piece(p), b_piece(e)

            @pl.when(q_in & (l > 0))
            def _():
                remote(bu_in.at[q], bu_in.at[q], bus.at[q], bur.at[q], lay=l).wait_recv()

            @pl.when(q_in & (l == 0))
            def _():
                bu_out[q] = own_ref[q]

            @pl.when(q_in & (l > 0) & (l < n - 1))
            def _():
                bu_out[q] = (own_ref[q].astype(F32) + bu_in[q].astype(F32)).astype(BF16)

            @pl.when(p_in_ & (l < n - 1))
            def _():
                remote(bd_in.at[p], bd_in.at[p], bds.at[p], bdr.at[p], lay=l).wait_recv()

            @pl.when(p_in_ & (l == n - 1))
            def _():
                bd_out[p] = own_ref[p]

            @pl.when(p_in_ & (l > 0) & (l < n - 1))
            def _():
                bd_out[p] = (own_ref[p].astype(F32) + bd_in[p].astype(F32)).astype(BF16)

            def error(total):
                c, i = e // b_steps, lax.rem(e, b_steps)
                t, i = i // cuts, lax.rem(i, cuts)
                over = pl.ds(pl.multiple_of(i * part, part), part)
                aim = t_ref[t, :, chunk(c), over].reshape(rows, part).astype(F32)
                e_ref[t, :, chunk(c), over] = ((total - aim) * scale).astype(BF16).reshape(w_count, ct, part)

            @pl.when(e_in & (l == 0))
            def _():
                error(own_ref[e].astype(F32) + bd_in[e].astype(F32))

            @pl.when(e_in & (l == n - 1))
            def _():
                error(own_ref[e].astype(F32) + bu_in[e].astype(F32))

            @pl.when(e_in & (l > 0) & (l < n - 1))
            def _():
                error(own_ref[e].astype(F32) + bu_in[e].astype(F32) + bd_in[e].astype(F32))

            @pl.when(q_in & (l < n - 1))
            def _():
                b_up(q).start()

            @pl.when(p_in_ & (l > 0))
            def _():
                b_dn(p).start()


        def x_send(c, i, v):
            where = pl.ds(i * g, g)
            return remote(x_out.at[c, v, where], x_in.at[c, w, where], xs.at[(c * groups + i) * w_count + v],
                          xr.at[(c * groups + i) * w_count + w], wid=v)

        def x_landed(c, i, v):
            where = pl.ds(i * g, g)
            return remote(x_in.at[c, v, where], x_in.at[c, v, where],
                          xs.at[(c * groups + i) * w_count + v],
                          xr.at[(c * groups + i) * w_count + v], wid=v)

        def slot_group(c, i):
            for k in [i * g + d for d in range(g)]:
                held = e_ref[tab[at.tgt + k], :, chunk(c), :].reshape(rows, width)
                back = lax.dot_general(
                    held, w_ref[k], (((1,), (1,)), ((), ())), preferred_element_type=F32
                ).astype(BF16).reshape(w_count, ct, block)
                for v in range(w_count):
                    x_out[c, v, k] = back[v]
            others(w, w_count, lambda v: x_send(c, i, v).start())

        def gather(c):
            def landed(i, carry):
                others(w, w_count, lambda v: x_landed(c, i, v).wait_recv())
                return carry

            lax.fori_loop(0, groups, landed, 0)

            def one(k, carry):
                total = c_sums[tab[at.prev_id + k]] + x_out[c, w, k].astype(F32)
                for d in range(1, w_count):
                    total = total + x_in[c, lax.rem(w + d, w_count), k].astype(F32)
                c_sums[k + 1] = total
                return carry

            lax.fori_loop(0, slots, one, 0)

            def out(b, carry):
                made[c, b] = c_sums[tab[at.last_id + b]].astype(BF16)
                return carry

            lax.fori_loop(0, blocks, out, 0)

        def z_up(q):
            return remote(zu_out.at[q], zu_in.at[q], zus.at[q], zur.at[q], lay=l + 1)

        def z_dn(q):
            return remote(zd_out.at[q], zd_in.at[q], zds.at[q], zdr.at[q], lay=l - 1)

        def z_inside(q):
            return (q >= 0) & (q < chunks * c_period) & (lax.rem(q + c_period * chunks, c_period) < z_steps)

        def z_piece(q):
            return q // c_period * z_steps + lax.rem(q + c_period * chunks, c_period)

        def own_z(q, dest):
            return made[q // z_steps, pl.ds(dest * per_dev + lax.rem(q, split) * pb, pb)].astype(F32)

        def twin_pre(c):
            return remote(twin_out.at[c], po_ref.at[r, chunk(c)], tps.at[c], tpr.at[c], rep=twin)

        def twin_landed(c):
            return remote(twin_out.at[c], po_ref.at[twin, chunk(c)], tps.at[c], tpr.at[c], rep=twin)

        def reduce_on(s):
            q, p = s - Z_SKEW * l, s - Z_SKEW * (n - 1 - l)
            q_in, p_in_ = z_inside(q), z_inside(p)
            q, p = z_piece(q), z_piece(p)
            to_up = n - 1 - lax.rem(q + z_pieces, z_steps) // split
            to_dn = lax.rem(p + z_pieces, z_steps) // split

            @pl.when(q_in & (l > 0) & (to_up >= l))
            def _():
                remote(zu_in.at[q], zu_in.at[q], zus.at[q], zur.at[q], lay=l).wait_recv()

            @pl.when(q_in & (l == 0))
            def _():
                zu_out[q] = own_z(q, to_up).astype(BF16)

            @pl.when(q_in & (l > 0) & (to_up > l))
            def _():
                zu_out[q] = (own_z(q, to_up) + zu_in[q].astype(F32)).astype(BF16)

            @pl.when(p_in_ & (l < n - 1) & (to_dn <= l))
            def _():
                remote(zd_in.at[p], zd_in.at[p], zds.at[p], zdr.at[p], lay=l).wait_recv()

            @pl.when(p_in_ & (l == n - 1))
            def _():
                zd_out[p] = own_z(p, to_dn).astype(BF16)

            @pl.when(p_in_ & (l < n - 1) & (to_dn < l))
            def _():
                zd_out[p] = (own_z(p, to_dn) + zd_in[p].astype(F32)).astype(BF16)

            off_up = (n - 1 - l) * split
            off_dn = l * split
            f = s - jnp.maximum(off_up + Z_SKEW * l, off_dn + Z_SKEW * (n - 1 - l))
            i = lax.rem(f + c_period * chunks, c_period)
            whole = (f >= 0) & (f < chunks * c_period) & (i < split)
            c = f // c_period

            def finish(total):
                blocks_here = pl.ds(i * pb, pb)
                grad = (total * sl_ref[blocks_here, chunk(c), :]).astype(BF16)
                if split == r_count:
                    @pl.when(i == r)
                    def _():
                        for b in range(pb):
                            po_ref[r, chunk(c), b * block:(b + 1) * block] = grad[b]

                    @pl.when(i != r)
                    def _():
                        for b in range(pb):
                            twin_out[c, :, b * block:(b + 1) * block] = grad[b]
                else:
                    for b in range(pb):
                        for side in range(r_count):
                            cut = grad[b][:, side * half:(side + 1) * half]

                            @pl.when(r == side)
                            def _():
                                po_ref[side, chunk(c), b * half:(b + 1) * half] = cut

                            @pl.when(r != side)
                            def _():
                                twin_out[c, :, b * half:(b + 1) * half] = cut

            def mid():
                return made[c, pl.ds(l * per_dev + i * pb, pb)].astype(F32)

            @pl.when(whole & (l == 0))
            def _():
                finish(mid() + zd_in[c * z_steps + off_dn + i].astype(F32))

            @pl.when(whole & (l == n - 1))
            def _():
                finish(mid() + zu_in[c * z_steps + off_up + i].astype(F32))

            @pl.when(whole & (l > 0) & (l < n - 1))
            def _():
                finish(mid() + zu_in[c * z_steps + off_up + i].astype(F32)
                       + zd_in[c * z_steps + off_dn + i].astype(F32))

            @pl.when(q_in & (to_up > l))
            def _():
                z_up(q).start()

            @pl.when(p_in_ & (to_dn < l))
            def _():
                z_dn(p).start()

            @pl.when(whole & (i == split - 1))
            def _():
                twin_pre(c).start()


        twins = [
            remote(lat_ref.at[:, :, :, pl.ds(pl.multiple_of(twin * half, half), half)], lo_ref.at[:, r],
                   ts.at[0], tr.at[0], rep=twin),
            remote(e_ref, eo_ref.at[:, r], ts.at[1], tr.at[1], rep=twin),
        ] + [
            remote(a_ref.at[v], ao_ref.at[lax.rem(v - w + w_count, w_count), r], ts.at[2 + v], tr.at[2 + v],
                   rep=twin)
            for v in range(w_count)
        ]
        mine = [
            pltpu.make_async_copy(
                lat_ref.at[:, :, :, pl.ds(pl.multiple_of(r * half, half), half)], lo_ref.at[:, r], asem.at[0]),
            pltpu.make_async_copy(e_ref, eo_ref.at[:, r], asem.at[1]),
        ] + [
            pltpu.make_async_copy(
                a_ref.at[v], ao_ref.at[lax.rem(v - w + w_count, w_count), r], asem.at[2 + v])
            for v in range(w_count)
        ]

        def tick(s, carry):
            def arrive(d):
                at_chunk(s, A_GATE + A_SKEW * d, a_period, lambda c: nearest(l, n, d, lambda j: take(c, j)))

            loop(1, n, arrive)
            hand_on(s - b_first)
            at_chunk(s, c_gather, c_period, gather)
            reduce_on(s - c_gather)
            at_chunk(s, A_GATE, a_period, gated)
            at_chunk(s, 0, p_period, product)

            @pl.when(s < a_decode - 1)
            def _():
                some_tables(s)

            t = s - c_slots

            @pl.when((t >= 0) & (t < chunks * c_period))
            def _():
                c, i = t // c_period, lax.rem(t, c_period)
                lax.fori_loop(
                    (i * groups + c_period - 1) // c_period, ((i + 1) * groups + c_period - 1) // c_period,
                    lambda j, z: (slot_group(c, j), z)[1], 0,
                )

            u = s - a_decode

            @pl.when((u >= 0) & (u < chunks * b_period))
            def _():
                c, i = u // b_period, lax.rem(u, b_period)

                @pl.when(i == 0)
                def _():
                    crossed(c)

                for d in range(per_step):
                    @pl.when(i * per_step + d < slots)
                    def _():
                        slot(i * per_step + d)

                @pl.when(i == b_period - 1)
                def _():
                    emit(c)

            @pl.when(s == a_decode - 1)
            def _():
                loop(0, slots, lambda k: weight(k).wait())
                aims.wait()
                for v in range(w_count):
                    twins[2 + v].start()
                    mine[2 + v].start()

            @pl.when(s == a_decode + (chunks - 1) * b_period)
            def _():
                twins[0].start()
                mine[0].start()

            @pl.when(s == c_slots + (chunks - 1) * c_period)
            def _():
                twins[1].start()
                mine[1].start()

            return carry

        lax.fori_loop(0, ticks, tick, 0)

        def a_sent(q, carry):
            goes(q // n, lax.rem(q, n), lambda copy: copy.wait_send())
            return carry

        lax.fori_loop(0, chunks * n, a_sent, 0)

        def b_sent(q, carry):
            @pl.when(l < n - 1)
            def _():
                b_up(q).wait_send()

            @pl.when(l > 0)
            def _():
                b_dn(q).wait_send()

            return carry

        lax.fori_loop(0, b_pieces, b_sent, 0)

        def z_sent(q, carry):
            to_up = n - 1 - lax.rem(q, z_steps) // split
            to_dn = lax.rem(q, z_steps) // split

            @pl.when(to_up > l)
            def _():
                z_up(q).wait_send()

            @pl.when(to_dn < l)
            def _():
                z_dn(q).wait_send()

            return carry

        lax.fori_loop(0, z_pieces, z_sent, 0)

        def x_sent(q, carry):
            others(w, w_count, lambda v: x_send(q // groups, lax.rem(q, groups), v).wait_send())
            return carry

        lax.fori_loop(0, chunks * groups, x_sent, 0)
        for c in range(chunks):
            for i in range(cols):
                others(w, w_count, lambda v: p_send(c, i, v).wait_send())
            twin_landed(c).wait()
        for copy in twins + mine:
            copy.wait()

    b_piece_shape = (b_pieces, rows, part)
    z_piece_shape = (z_pieces, pb, ct, block)
    x_shape = (chunks, w_count, slots, ct, block)
    lat_shape = (blocks, w_count, toks, block)
    vmem = pl.BlockSpec(memory_space=pltpu.VMEM)
    smem = pl.BlockSpec(memory_space=pltpu.SMEM)
    dma = pltpu.SemaphoreType.DMA
    x_sems = chunks * groups * w_count
    return pl.pallas_call(
        body,
        out_shape=(
            jax.ShapeDtypeStruct((at.size,), jnp.int32),
            jax.ShapeDtypeStruct((r_count, toks, columns), BF16),
            jax.ShapeDtypeStruct((blocks, r_count, w_count, toks, half), BF16),
            jax.ShapeDtypeStruct((layers, r_count, w_count, toks, width), BF16),
            jax.ShapeDtypeStruct((w_count, r_count, toks, width), BF16),
        ),
        in_specs=[smem, ANY, ANY, vmem, vmem, ANY, ANY],
        out_specs=(smem, vmem, ANY, ANY, ANY),
        scratch_shapes=[
            pltpu.VMEM((w_count, toks, width), BF16),
            pltpu.VMEM(enc_weight.shape, BF16),
            pltpu.VMEM((w_count * toks, per_dev), F32),
            pltpu.VMEM(targets.shape, BF16),
            pltpu.VMEM(dec_weight.shape, BF16),
            pltpu.VMEM(lat_shape, BF16),
            pltpu.VMEM((blocks, w_count, ct, block), BF16),
            pltpu.VMEM((per_dev, toks, block), F32),
            pltpu.VMEM((chunks, w_count, ct, lat_dev), BF16),
            pltpu.VMEM((chunks, w_count, ct, lat_dev), BF16),
            pltpu.VMEM(targets.shape, BF16),
            pltpu.VMEM((slots + 1, rows, width), F32),
        ] + [pltpu.VMEM(b_piece_shape, BF16)] * 5 + [
            pltpu.VMEM(x_shape, BF16),
            pltpu.VMEM(x_shape, BF16),
            pltpu.VMEM((slots + 1, ct, block), F32),
            pltpu.VMEM((chunks, blocks, ct, block), BF16),
        ] + [pltpu.VMEM(z_piece_shape, BF16)] * 4 + [
            pltpu.VMEM((chunks, ct, columns), BF16),
            dma((slots,)), dma((chunks * cols * w_count,)), dma((chunks * cols * w_count,)),
        ] + [dma((chunks * n,))] * 3 + [dma((chunks * n * w_count,))] * 2 + [dma((b_pieces,))] * 4
        + [dma((x_sems,))] * 2 + [dma((z_pieces,))] * 4 + [
            dma((2 + w_count,)), dma((2 + w_count,)), dma((chunks,)), dma((chunks,)), dma((2 + w_count,)),
            dma((2 + lat_dev // wide,)),
        ],
        compiler_params=pltpu.CompilerParams(
            collective_id=cid, has_side_effects=True, vmem_limit_bytes=67043328
        ),
        name="step",
    )(dec_list, acts, enc_weight, enc_bias, gate, dec_weight, targets)


def decoder_grads(tables, lat, err, slots):
    layers, toks, width = err.shape
    blocks, _, half = lat.shape
    g = group_of(slots)
    at = Tables(slots, layers, blocks)

    def body(tab, l_ref, e_ref, o_ref):
        for i in range(g):
            k = pl.program_id(0) * g + i

            @pl.when(tab[at.raw + k] >= 0)
            def _():
                o_ref[i] = lax.dot_general(
                    l_ref[tab[at.id + k]], e_ref[tab[at.tgt + k]], (((0,), (0,)), ((), ())),
                    preferred_element_type=F32,
                )

            @pl.when(tab[at.raw + k] < 0)
            def _():
                o_ref[i] = jnp.zeros_like(o_ref[i])

    return slot_call(
        body, (tables,), (lat, err),
        [pl.BlockSpec((blocks, toks, half), lambda k, t: (0, 0, 0)),
         pl.BlockSpec((layers, toks, width), lambda k, t: (0, 0, 0))],
        jax.ShapeDtypeStruct((slots, half, width), F32),
        pl.BlockSpec((g, half, width), lambda k, t: (k, 0, 0)),
        [], 2 * slots * toks * half * width, "decoder_grads", slots // g,
    )


def local(acts, targets, enc_weight, enc_bias, gate_mask, dec_list, dec_weight):
    layers, tok_rows, width = acts.shape
    lat_dev = enc_weight.shape[1]
    slots, block, _ = dec_weight.shape
    w_count, r_count = lax.axis_size("wid"), lax.axis_size("rep")
    shape = (layers, w_count, tok_rows // w_count, width)
    scale = float(tok_rows * r_count) ** (-0.5)
    tables, pre_mine, lat, err, acts_all = step(
        acts.reshape(shape), enc_weight, enc_bias.reshape(1, lat_dev), gate_mask.T, dec_list.T,
        dec_weight, targets.reshape(shape), scale, 0,
    )
    pre_all = [pre_mine] + [
        lax.ppermute(pre_mine, "wid", [(i, (i - d) % w_count) for i in range(w_count)])
        for d in range(1, w_count)
    ]
    everyone = r_count * tok_rows
    dec_out = decoder_grads(
        tables, lat.reshape(lat.shape[0], everyone, block // r_count), err.reshape(layers, everyone, width),
        slots,
    )
    pre_all = jnp.stack(pre_all).reshape(everyone, lat_dev // r_count)
    enc_out = lax.dot_general(
        acts_all.reshape(everyone, width), pre_all, (((0,), (0,)), ((), ())), preferred_element_type=F32
    )
    bias_out = jnp.sum(pre_all.astype(F32), axis=0)
    return (enc_out, bias_out, dec_out)


def solution(mesh):
    return jax.shard_map(
        local,
        mesh=mesh,
        in_specs=(
            P(None, ("grp", "rep"), "wid"),
            P(None, ("grp", "rep"), "wid"),
            P("wid", "lay"),
            P("lay"),
            P(("grp", "rep"), "lay"),
            P("lay", None),
            P("lay", None, "wid"),
        ),
        out_specs=(
            P(("grp", "wid"), ("lay", "rep")),
            P(("grp", "lay", "rep")),
            P(("grp", "lay"), "rep", "wid"),
        ),
        check_vma=False,
    )
```
